256 devices in a mesh: grp: 8 (over y_hi, x), frag: 32 (over y_lo, z, core).
Axes of the slice: x: 4, y: 4 (y_hi: 2, y_lo: 2; y = y_hi * 2 + y_lo), z: 8, core: 2. Of those that a mesh axis runs over, the one named last changes fastest.
Arguments:
- density: bfloat16 [256, 9216], P('frag'), may hold values from -0.1 to 1, as said below
- fock_blocks: bfloat16 [256, 9216], P('frag'), may hold values from -8 to 8, as said below
- coupling: bfloat16 [1024, 9216], P(('grp', 'frag')), may hold values from -1.796875 to 1.796875
- dimer_pairs: int32 [1024, 2], P(('grp', 'frag')), may hold values from 0 to 255, as said below
- atom_counts: int32 [256], P('frag'), may hold values from 8 to 16
- nuclear_charge: float32 [4096], P('frag'), may hold values from 4 to 12
- coords: float32 [3, 4096], P(None, 'frag'), may hold values from -120 to 120
Outputs:
- density_correction: float32 [256, 9216], P('frag')
- dimer_energy: float32 [1024], P(('grp', 'frag'))
- total_energy: float32 [], replicated
The draws below stay inside these ranges and needn't reach their ends.
Inputs may be any that keep to these rules, and one draw needn't show every extreme that they name: `dimer_pairs`: dimer d has fragments I < J; I // 8 == (d // 4) % 32, and J // 8 lies between I // 8 and I // 8 + 3. `density`: each row is a symmetric matrix. `fock_blocks`: each row is a symmetric matrix.
All inputs are finite; a program needn't handle non-finite values. Where the reference program divides by a largest or mean magnitude, that divisor is 1e-20 or more.
Results may differ from the reference program's by a relative error of at most 0.0018.
Values may be sent and summed in bfloat16 or wider, within the bound.
No kernel may reach another device: no remote copies, remote signals or barrier semaphores. Data moves between devices by JAX's collectives and lax.ppermute only.
A program may use at most 64 MiB of HBM per device.

```python
import jax
import jax.numpy as jnp
from jax import lax

NB = 96
NA = 16
REACH = 3
PURIF = 12
FRAG_DEV = 8
DIM_DEV = 4
NFRAG = 256
DIMERS = 1024
ATOMS = 4096
N_FRAG = 32


def symmetric_rows(key_main, off_scale, diag_lo, diag_hi):
    key_off, key_diag = jax.random.split(key_main)
    off_noise = off_scale * jax.random.normal(key_off, (NFRAG, NB, NB), jnp.float32)
    occupancy = jax.random.uniform(key_diag, (NFRAG, NB), jnp.float32, diag_lo, diag_hi)
    symmetric = (off_noise + jnp.swapaxes(off_noise, 1, 2)) * 0.7071
    small_eye = jnp.eye(NB, dtype=jnp.float32)[None, :, :]
    blocks = symmetric * (1.0 - small_eye) + occupancy[:, :, None] * small_eye
    return blocks.reshape(NFRAG, NB * NB)


def draw_density(key, part):
    return symmetric_rows(jax.random.fold_in(key, 3), 0.01, 0.15, 0.85).astype(jnp.bfloat16)


def draw_fock_blocks(key, part):
    return symmetric_rows(jax.random.fold_in(key, 5), 0.3, -4.0, 4.0).astype(jnp.bfloat16)


def draw_dimer_pairs(key, part):
    key_first, key_step, key_far = jax.random.split(jax.random.fold_in(key, 11), 3)
    row_index = jnp.arange(DIMERS, dtype=jnp.int32)
    column = row_index // DIM_DEV % N_FRAG
    slot_index = row_index % DIM_DEV
    is_last = (column == N_FRAG - 1).astype(jnp.int32)
    first_local = jax.random.randint(key_first, (DIMERS,), 0, FRAG_DEV - is_last)
    first_frag = column * FRAG_DEV + first_local
    step_size = jax.random.randint(key_step, (DIMERS,), 0, REACH * FRAG_DEV)
    second = jnp.minimum(first_frag + 1 + step_size, NFRAG - 1)
    far_frag = (column + REACH) * FRAG_DEV + jax.random.randint(key_far, (DIMERS,), 0, FRAG_DEV)
    pick_far = jnp.logical_and(slot_index == 0, column + REACH < N_FRAG)
    second = jnp.where(pick_far, far_frag, second)
    return jnp.stack([first_frag, second], axis=1).astype(jnp.int32)


def plant(drawn, key, smallest, top_value):
    longest = drawn.shape.index(max(drawn.shape))
    spots = []
    for shift in (0, 1):
        where = [jax.random.randint(jax.random.fold_in(key, axis), (), 0, length) for axis, length in enumerate(drawn.shape)]
        where[longest] = (where[longest] + shift) % drawn.shape[longest]
        spots.append(tuple(where))
    return drawn.at[spots[0]].set(smallest).at[spots[1]].set(top_value)


def levels(rng, extent, cuts, least, largest):
    level, own = 1.0, jax.random.fold_in(rng, 6)
    for dim, blocks in cuts:
        draws = jnp.exp(jax.random.uniform(jax.random.fold_in(own, dim), (blocks,), jnp.float32, least / len(cuts), largest / len(cuts)))
        level = level * jnp.repeat(draws, extent[dim] // blocks).reshape([-1 if axis == dim else 1 for axis in range(len(extent))])
    return level


def normal_values(rng, shape, scale, bound, cuts=(), kind=jnp.bfloat16):
    entries = scale * jax.random.normal(rng, shape, jnp.float32)
    if cuts:
        entries = entries * levels(rng, shape, cuts, -0.22, 0.18)
    return jnp.clip(entries, -bound, bound).astype(kind)


def setup_inputs(seed: int = 0) -> dict:
    key_list = jax.random.split(jax.random.key(seed), 8)
    return {
        "density": draw_density(jax.random.fold_in(key_list[7], 71), 0),
        "fock_blocks": draw_fock_blocks(jax.random.fold_in(key_list[7], 71), 0),
        "coupling": normal_values(key_list[2], (DIMERS, NB * NB), 0.3, 1.796875, ((0, 256),)),
        "dimer_pairs": draw_dimer_pairs(jax.random.fold_in(key_list[7], 71), 0),
        "atom_counts": plant(jax.random.randint(key_list[4], (NFRAG,), NA // 2, NA + 1), jax.random.fold_in(key_list[4], 1), NA // 2, NA).astype(jnp.int32),
        "nuclear_charge": jnp.clip(4.0 + 8.0 * jax.random.uniform(key_list[5], (ATOMS,), jnp.float32) ** levels(key_list[5], (ATOMS,), ((0, 32),), -0.2, 0.2), 4.0, 12.0),
        "coords": normal_values(key_list[6], (3, ATOMS), 20.0, 120.0, ((1, 32),), jnp.float32),
    }


FULL_PRECISION = lax.Precision.HIGHEST

def basis_atoms(count_real):
    basis_index = jnp.arange(NB, dtype=jnp.float32)[None, :, None]
    atom_index = jnp.arange(NA, dtype=jnp.float32)[None, None, :]
    scaled = basis_index * count_real[:, None, None]
    inside = jnp.logical_and(atom_index * NB <= scaled, scaled < (atom_index + 1.0) * NB)
    return inside.astype(jnp.float32)

def atom_table(density, nuclear_charge, atom_counts, coords):
    frag_count = density.shape[0]
    count_real = atom_counts.astype(jnp.float32)
    owners = basis_atoms(count_real)
    blocks = density.reshape(frag_count, NB, NB).astype(jnp.float32)
    on_diagonal = jnp.diagonal(blocks, axis1=1, axis2=2)
    population = 2.0 * lax.optimization_barrier(jnp.sum(on_diagonal[:, :, None] * owners, axis=1))
    is_live = (jnp.arange(NA, dtype=jnp.float32)[None, :] < count_real[:, None]).astype(jnp.float32)
    charge = is_live * nuclear_charge.reshape(frag_count, NA) - population
    return jnp.concatenate([charge.reshape(1, -1), coords, is_live.reshape(1, -1)], axis=0)

def embed_potential(receivers, pair_ids, atom_rows):
    source_frag = jnp.arange(atom_rows.shape[1], dtype=jnp.int32) // NA
    keep_mask = jnp.logical_and(source_frag != pair_ids[0], source_frag != pair_ids[1]).astype(jnp.float32)
    offsets = receivers[1:4, :, None] - atom_rows[1:4, None, :]
    distance_sq = lax.optimization_barrier(jnp.sum(offsets * offsets, axis=0))
    return lax.optimization_barrier(jnp.sum((keep_mask * atom_rows[0])[None, :] / jnp.sqrt(distance_sq + 1.0), axis=1))

def dimer_solve(dens_pair, fock_pair, coupling_row, potential, count_pair):
    owners = basis_atoms(count_pair)
    site_shift = lax.optimization_barrier(jnp.sum(owners * potential.reshape(2, 1, NA), axis=2))
    dens_blocks = dens_pair.astype(jnp.float32).reshape(2, NB, NB)
    fock_parts = fock_pair.astype(jnp.float32).reshape(2, NB, NB)
    cross_block = coupling_row.astype(jnp.float32).reshape(NB, NB)
    small_eye = jnp.eye(NB, dtype=jnp.float32)
    top_rows = jnp.concatenate([fock_parts[0] + small_eye * site_shift[0][None, :], cross_block], axis=1)
    low_rows = jnp.concatenate([cross_block.T, fock_parts[1] + small_eye * site_shift[1][None, :]], axis=1)
    dimer_fock = jnp.concatenate([top_rows, low_rows], axis=0)
    identity = jnp.eye(2 * NB, dtype=jnp.float32)
    centre = jnp.trace(dimer_fock) / (2.0 * NB)
    shifted = dimer_fock - centre * identity
    width = jnp.max(lax.optimization_barrier(jnp.sum(jnp.abs(shifted), axis=1))) + 1e-06
    start = 0.5 * identity - shifted / (2.0 * width)

    def purify(index, current):
        square = jnp.dot(current, current, precision=FULL_PRECISION)
        return 3.0 * square - 2.0 * jnp.dot(square, current, precision=FULL_PRECISION)
    purified = lax.fori_loop(0, PURIF, purify, start)
    zero_block = jnp.zeros((NB, NB), jnp.float32)
    start_guess = jnp.concatenate([jnp.concatenate([dens_blocks[0], zero_block], axis=1), jnp.concatenate([zero_block, dens_blocks[1]], axis=1)], axis=0)
    energy = jnp.sum((purified - start_guess) * dimer_fock.T)
    changes = jnp.stack([purified[:NB, :NB] - dens_blocks[0], purified[NB:, NB:] - dens_blocks[1]])
    return (changes.reshape(2, NB * NB), energy)

def reference(density, fock_blocks, coupling, dimer_pairs, atom_counts, nuclear_charge, coords):
    atom_rows = atom_table(density, nuclear_charge, atom_counts, coords)

    def solve_one(dimer_item):
        pair_ids, coupling_row = dimer_item
        columns = (pair_ids[:, None] * NA + jnp.arange(NA, dtype=jnp.int32)[None, :]).reshape(-1)
        receivers = jnp.take(atom_rows, columns, axis=1)
        potential = embed_potential(receivers, pair_ids, atom_rows)
        count_pair = lax.optimization_barrier(jnp.sum(receivers[4].reshape(2, NA), axis=1))
        return dimer_solve(jnp.take(density, pair_ids, axis=0), jnp.take(fock_blocks, pair_ids, axis=0), coupling_row, potential, count_pair)
    changes, energies = lax.map(solve_one, (dimer_pairs, coupling))
    flat_blocks = changes.reshape(-1, NB * NB)
    fragment_ids = dimer_pairs.reshape(-1)
    density_correction = jax.ops.segment_sum(flat_blocks, fragment_ids, num_segments=NFRAG)
    return (density_correction, energies, jnp.sum(energies))
```

```python
import jax
import jax.numpy as jnp
from jax import lax
from jax.experimental import pallas as pl
from jax.experimental.pallas import tpu as pltpu
from jax.sharding import Mesh
from jax.sharding import PartitionSpec as P

NB = 96
NA = 16
REACH = 3
PURIF = 12
FRAG_DEV = 8
DIM_DEV = 4
FLAT = NB * NB
FRAG = ("frag_0", "frag_1", "frag_2")
PAIR = ("frag_0", "frag_1")
GRP_FRAG = ("grp_0", "grp_1", "frag_0", "frag_1", "frag_2")
TEAM = ("grp_0", "grp_1", "frag_2")
N_FRAG = 32
N_PAIR = 16
N_TEAM = 16
N_GRP = 8
F32 = jnp.float32
BF16 = jnp.bfloat16
VMEM = pltpu.VMEM
SMEM = pltpu.SMEM

ID_LANE = 96
ONE_LANE = 97
ENERGY_LANE = 98
SUM_LANE = 99


def iota(shape, dim):
    return lax.broadcasted_iota(jnp.int32, shape, dim)


def exchange(value, axis):
    return lax.all_to_all(value, axis, split_axis=0, concat_axis=0, tiled=True)


def dot32(left, right):
    return jnp.dot(left, right, preferred_element_type=F32)


def halves(value):
    high = value.astype(BF16)
    return high, (value - high.astype(F32)).astype(BF16)


def table_kernel(counts, dens, fock, nuclear, coords, table):
    lane = iota((1, 128), 1)
    trace_sum = jnp.zeros((FRAG_DEV, 128), F32)
    diagonal = jnp.zeros((FRAG_DEV, 128), F32)
    for chunk in range(FLAT // 128):
        here = slice(chunk * 128, (chunk + 1) * 128)
        block = dens[:, here].astype(F32)
        trace_sum += block * fock[:, here].astype(F32)
        first = (-chunk * 128) % (NB + 1)
        on_diagonal = jnp.logical_or(lane == first, lane == first + NB + 1)
        diagonal += jnp.where(on_diagonal, block, 0.0)
    fragment = lane // NA
    atom = (lane % NA).astype(F32)
    count = jnp.zeros((1, 128), F32)
    for index in range(FRAG_DEV):
        count = jnp.where(fragment == index, counts[index].astype(F32), count)
    basis = (iota((128, 128), 0) * 33) % 128
    scaled = basis.astype(F32) * count
    inside = jnp.logical_and(atom * NB <= scaled, scaled < (atom + 1.0) * NB)
    owner = jnp.where(jnp.logical_and(inside, basis < NB), 1.0, 0.0).astype(BF16)
    spread = dot32(diagonal.astype(BF16), owner)
    own_lane = iota((FRAG_DEV, 128), 0) == fragment
    population = jnp.sum(jnp.where(own_lane, spread, 0.0), axis=0, keepdims=True)
    traces = jnp.sum(trace_sum, axis=1, keepdims=True)
    at_first = jnp.logical_and(own_lane, lane % NA == 0)
    trace_row = jnp.sum(jnp.where(at_first, traces, 0.0), axis=0, keepdims=True)
    live = jnp.where(atom < count, 1.0, 0.0)
    charge = live * nuclear[...] - 2.0 * population
    row = iota((8, 128), 0)
    rows = [charge, coords[0:1, :], coords[1:2, :], coords[2:3, :], count, population, trace_row]
    value = jnp.zeros((8, 128), F32)
    for index, content in enumerate(rows):
        value = jnp.where(row == index, content, value)
    for peer in range(N_FRAG):
        table[peer] = value


def atom_table(density, fock_blocks, nuclear_charge, atom_counts, coords):
    return pl.pallas_call(
        table_kernel,
        out_shape=jax.ShapeDtypeStruct((N_FRAG, 8, 128), F32),
        in_specs=[pl.BlockSpec(memory_space=SMEM)] + [pl.BlockSpec(memory_space=VMEM)] * 4,
        out_specs=pl.BlockSpec(memory_space=VMEM),
        name="atom_table",
    )(atom_counts, density, fock_blocks, nuclear_charge.reshape(1, 128), coords)


def solve_kernel(
    pairs, table, fock_0, fock_1, fock_2, fock_3, coupling, sent, energies,
    columns, masked, fock_j, shifted, state, high, low, square_high, square_low,
):
    focks = (fock_0, fock_1, fock_2, fock_3)
    base = (pairs[0] // FRAG_DEV) * FRAG_DEV
    pair_base = (base // NA) * NA
    lane = iota((NA, 128), 1)
    atom = iota((NA, 128), 0).astype(F32)

    shifted[...] = jnp.zeros_like(shifted)
    for buffer in (high, low, square_high, square_low):
        for dimer in range(DIM_DEV):
            buffer[dimer, NB:128, :] = jnp.zeros((128 - NB, 256), BF16)
            buffer[dimer, 128 + NB :, :] = jnp.zeros((128 - NB, 256), BF16)

    source = iota((N_FRAG, 128), 0) * FRAG_DEV + iota((N_FRAG, 128), 1) // NA
    charges = table[:, 0, :]
    for dimer in range(DIM_DEV):
        first, second = pairs[2 * dimer], pairs[2 * dimer + 1]
        hidden = jnp.logical_or(source == first, source == second)
        masked[dimer] = jnp.where(hidden, 0.0, charges)
        for side in range(2):
            fragment = pairs[2 * dimer + side]
            columns[2 * dimer + side] = table[fragment // FRAG_DEV].T

    shifts, starts = [], []
    for dimer in range(DIM_DEV):
        own, places = [], []
        for side in range(2):
            local = pl.multiple_of((pairs[2 * dimer + side] % FRAG_DEV) * NA, NA)
            mine = columns[2 * dimer + side, pl.ds(local, NA), :]
            own.append(mine)
            places.append([jnp.broadcast_to(mine[:, k : k + 1], (NA, 128)) for k in (1, 2, 3)])

        def gather(step, sums, dimer=dimer, places=places):
            sums = list(sums)
            for inner in range(4):
                block = step * 4 + inner
                weight = masked[dimer, pl.ds(block, 1), :]
                spot = [table[block, k : k + 1, :] for k in (1, 2, 3)]
                for side in range(2):
                    delta = [place - here for place, here in zip(places[side], spot)]
                    distance = delta[0] * delta[0] + delta[1] * delta[1] + delta[2] * delta[2]
                    sums[side] += weight * lax.rsqrt(distance + 1.0)
            return tuple(sums)

        zero = jnp.zeros((NA, 128), F32)
        sums = lax.fori_loop(0, N_FRAG // 4, gather, (zero, zero))
        start = jnp.zeros((1, 1), F32)
        for side in range(2):
            potential = jnp.sum(sums[side], axis=1, keepdims=True)
            count, population, trace = (own[side][:, k : k + 1] for k in (4, 5, 6))
            scaled = lane.astype(F32) * count
            inside = jnp.logical_and(atom * NB <= scaled, scaled < (atom + 1.0) * NB)
            inside = jnp.logical_and(inside, lane < NB)
            shifts.append(jnp.sum(jnp.where(inside, potential, 0.0), axis=0, keepdims=True))
            start += jnp.sum(potential * population + trace, axis=0, keepdims=True)
        starts.append(start)

    small_eye = iota((NB, NB), 0) == iota((NB, NB), 1)
    rows, cols = iota((2 * NB, 256), 0), iota((2 * NB, 256), 1)
    eye = cols == jnp.where(rows < NB, rows, rows + (128 - NB))
    centres, widths = [], []
    for dimer in range(DIM_DEV):
        second = pairs[2 * dimer + 1] - base
        for far in range(REACH + 1):

            @pl.when(second // FRAG_DEV == far)
            def _(far=far, second=second):
                fock_j[...] = focks[far][second % FRAG_DEV]

        cross = coupling[dimer].astype(F32)
        for side in range(2):
            at, to = side * NB, side * 128
            part = fock_0[pairs[2 * dimer] - base] if side == 0 else fock_j[...]
            shift = shifts[2 * dimer + side][:, :NB]
            shifted[dimer, at : at + NB, to : to + NB] = part.astype(F32) + jnp.where(
                small_eye, shift, 0.0
            )
        shifted[dimer, :NB, 128 : 128 + NB] = cross
        shifted[dimer, NB:, :NB] = cross.T
        fock = shifted[dimer]
        trace = jnp.sum(jnp.where(eye, fock, 0.0), axis=(0, 1), keepdims=True)
        centre = trace / (2.0 * NB)
        fock = jnp.where(eye, fock - centre, fock)
        width = jnp.max(jnp.sum(jnp.abs(fock), axis=1, keepdims=True), axis=0, keepdims=True) + 1e-06
        shifted[dimer] = fock
        start = fock / width
        state[dimer] = start
        keep(high, low, dimer, start)
        centres.append(centre)

    def purify(step, carry):
        for dimer in range(DIM_DEV):
            square = product(high, low, dimer, high, low)
            keep(square_high, square_low, dimer, square)
        for dimer in range(DIM_DEV):
            cube = product(high, low, dimer, square_high, square_low)
            later = 1.5 * state[dimer] - 0.5 * cube
            state[dimer] = later
            keep(high, low, dimer, later)
        return carry

    lax.fori_loop(0, PURIF, purify, 0)

    last = jnp.zeros((1, 128), F32)
    row_lane = iota((1, 128), 1)
    lane_16 = iota((16, 128), 1)
    for dimer in range(DIM_DEV):
        final = state[dimer]
        overlap = jnp.sum(final * shifted[dimer], axis=(0, 1), keepdims=True)
        trace = jnp.sum(jnp.where(eye, final, 0.0), axis=(0, 1), keepdims=True)
        centre = centres[dimer]
        energy = 0.5 * (2.0 * NB * centre - overlap - centre * trace) - starts[dimer]
        last = jnp.where(row_lane == dimer, energy, last)
        for side in range(2):
            slot = side * DIM_DEV + dimer
            block = final[side * NB : (side + 1) * NB, side * 128 : (side + 1) * 128]
            corner = pltpu.roll(block[64:96, :], 32, 1)
            target = (pairs[2 * dimer + side] - pair_base).astype(F32)
            beside = jnp.where(lane_16 == ID_LANE, target, 0.0)
            beside = jnp.where(lane_16 == ONE_LANE, 1.0, beside)
            if side == 0:
                beside = jnp.where(lane_16 == ENERGY_LANE, energy, beside)
            for part in range(4):
                piece = block[16 * part : 16 * (part + 1), :]
                other = corner[16 * part : 16 * (part + 1), :] if part < 2 else beside
                piece = jnp.where(lane_16 < NB, piece, other)
                sent[pl.ds(part * 8 + slot, 16, stride=32), :] = piece
    energies[...] = last


def keep(high, low, dimer, value):
    upper, lower = halves(value)
    for buffer, part in ((high, upper), (low, lower)):
        buffer[dimer, :NB, :] = part[:NB]
        buffer[dimer, 128 : 128 + NB, :] = part[NB:]


def product(high, low, dimer, right_high, right_low):
    upper = [high[dimer, :NB, :], high[dimer, 128 : 128 + NB, :]]
    lower = [low[dimer, :NB, :], low[dimer, 128 : 128 + NB, :]]
    both = dot32(jnp.concatenate(upper + lower, axis=0), right_high[dimer])
    cross = dot32(jnp.concatenate(upper, axis=0), right_low[dimer])
    return both[: 2 * NB] + (both[2 * NB :] + cross)


def solve_dimers(pairs, table, focks, coupling):
    matrix = (DIM_DEV, 2 * NB, 256)
    split = (DIM_DEV, 256, 256)
    return pl.pallas_call(
        solve_kernel,
        out_shape=(
            jax.ShapeDtypeStruct((N_TEAM * 32, 128), F32),
            jax.ShapeDtypeStruct((1, 128), F32),
        ),
        in_specs=[pl.BlockSpec(memory_space=SMEM)] + [pl.BlockSpec(memory_space=VMEM)] * 6,
        out_specs=(pl.BlockSpec(memory_space=VMEM), pl.BlockSpec(memory_space=VMEM)),
        scratch_shapes=[
            VMEM((2 * DIM_DEV, 128, 8), F32),
            VMEM((DIM_DEV, N_FRAG, 128), F32),
            VMEM((NB, NB), BF16),
            VMEM(matrix, F32),
            VMEM(matrix, F32),
            VMEM(split, BF16),
            VMEM(split, BF16),
            VMEM(split, BF16),
            VMEM(split, BF16),
        ],
        name="solve_dimers",
    )(pairs.reshape(2 * DIM_DEV), table, *focks, coupling)


def sort_kernel(arrived, own, next_1, next_2, energy):
    parts = [
        arrived[:, part * 8 : (part + 1) * 8, :].reshape(N_TEAM * 8, 128) for part in range(4)
    ]
    target = parts[2][:, ID_LANE : ID_LANE + 1].astype(jnp.int32)
    chosen = jnp.where(iota((128, 64), 1) == target, 1.0, 0.0).astype(BF16)
    value = jnp.concatenate(parts, axis=1)
    upper = value.astype(BF16)
    rest = value - upper.astype(F32)
    middle = rest.astype(BF16)
    lower = (rest - middle.astype(F32)).astype(BF16)
    total = jnp.zeros((64, 512), F32)
    for piece in (lower, middle, upper):
        total += lax.dot_general(
            chosen, piece, (((0,), (0,)), ((), ())), preferred_element_type=F32
        )
    own[...] = total[:16]
    next_1[...] = total[16:32].astype(BF16)
    next_2[...] = total[32:48].astype(BF16)
    summed = jnp.sum(parts[2], axis=0, keepdims=True)
    energy[...] = jnp.broadcast_to(summed, (8, 128))


def sort_blocks(arrived):
    return pl.pallas_call(
        sort_kernel,
        out_shape=(
            jax.ShapeDtypeStruct((16, 512), F32),
            jax.ShapeDtypeStruct((16, 512), BF16),
            jax.ShapeDtypeStruct((16, 512), BF16),
            jax.ShapeDtypeStruct((8, 128), F32),
        ),
        in_specs=[pl.BlockSpec(memory_space=VMEM)],
        out_specs=(pl.BlockSpec(memory_space=VMEM),) * 4,
        name="sort_blocks",
    )(arrived)


def join_kernel(own, from_1, from_2, energy, sent):
    total = own[...] + from_1[...].astype(F32) + from_2[...].astype(F32)
    lane = iota((8, 128), 1)
    mine = jnp.broadcast_to(energy[0:1, ENERGY_LANE : ENERGY_LANE + 1], (8, 128))
    for core in range(2):
        for part in range(4):
            rows = total[core * 8 : core * 8 + 8, part * 128 : (part + 1) * 128]
            if part == 2:
                rows = jnp.where(lane == SUM_LANE, mine, rows)
            for group in range(N_GRP):
                sent[2 * group + core, part * 8 : (part + 1) * 8, :] = rows


def join_blocks(own, from_1, from_2, energy):
    return pl.pallas_call(
        join_kernel,
        out_shape=jax.ShapeDtypeStruct((N_TEAM, 32, 128), F32),
        in_specs=[pl.BlockSpec(memory_space=VMEM)] * 4,
        out_specs=pl.BlockSpec(memory_space=VMEM),
        name="join_blocks",
    )(own, from_1, from_2, energy)


def unpack_kernel(arrived, dens, out, total, turned):
    for fragment in range(FRAG_DEV):
        upper = jnp.concatenate(
            [
                arrived[pl.ds(part * 8 + fragment, 16, stride=32), :]
                for part in range(4)
            ],
            axis=0,
        )
        turned[pl.ds(fragment, 32, stride=8), :] = jnp.concatenate(
            [upper.T[64:96, :], jnp.zeros((32, 64), F32)], axis=1
        )
    lane = iota((8, 128), 1)
    number = arrived[16:24, ONE_LANE : ONE_LANE + 1]
    number = jnp.broadcast_to(number, (8, 128))
    half_number = 0.5 * number

    def packed(row):
        start = (row % 16) * 32 + (row // 16) * 8
        return arrived[start : start + 8, :]

    def matrix_row(row):
        if row < 64:
            return packed(row)
        left = turned[(row - 64) * 8 : (row - 64) * 8 + 8, :]
        right = pltpu.roll(packed(row - 64), 96, 1)
        return jnp.where(lane < 64, left, right)

    def finish(tile, value):
        here = slice(tile * 128, (tile + 1) * 128)
        first = (-tile * 128) % (NB + 1)
        on_diagonal = jnp.logical_or(lane == first, lane == first + NB + 1)
        value = -0.5 * value - number * dens[:, here].astype(F32)
        out[:, here] = value + jnp.where(on_diagonal, half_number, 0.0)

    for quad in range(NB // 4):
        row_0 = matrix_row(4 * quad)
        row_1 = pltpu.roll(matrix_row(4 * quad + 1), 96, 1)
        row_2 = pltpu.roll(matrix_row(4 * quad + 2), 64, 1)
        row_3 = pltpu.roll(matrix_row(4 * quad + 3), 32, 1)
        finish(3 * quad, jnp.where(lane < 96, row_0, row_1))
        finish(3 * quad + 1, jnp.where(lane < 64, row_1, row_2))
        finish(3 * quad + 2, jnp.where(lane < 32, row_2, row_3))

    energy = jnp.zeros((1, 128), F32)
    for member in range(N_TEAM):
        energy += arrived[member * 32 + 16 : member * 32 + 17, :]
    total[...] = energy[:, SUM_LANE : SUM_LANE + 1]


def unpack_blocks(arrived, density):
    return pl.pallas_call(
        unpack_kernel,
        out_shape=(
            jax.ShapeDtypeStruct((FRAG_DEV, FLAT), F32),
            jax.ShapeDtypeStruct((1, 1), F32),
        ),
        in_specs=[pl.BlockSpec(memory_space=VMEM)] * 2,
        out_specs=(pl.BlockSpec(memory_space=VMEM),) * 2,
        scratch_shapes=[VMEM((256, 128), F32)],
        name="unpack_blocks",
    )(arrived.reshape(N_TEAM * 32, 128), density)


def energy_moves():
    moves = []
    for group in range(N_GRP):
        for pair in range(N_PAIR):
            for core in range(2):
                source = group * N_FRAG + pair * 2 + core
                away = (pair + 2 * group + core) % N_PAIR
                moves.append((source, group * N_FRAG + away * 2 + core))
    return moves


def per_device(density, fock_blocks, coupling, dimer_pairs, atom_counts, nuclear_charge, coords):
    table = atom_table(density, fock_blocks, nuclear_charge, atom_counts, coords)
    focks = [fock_blocks]
    for distance in range(1, REACH + 1):
        moves = [(index + distance, index) for index in range(N_FRAG - distance)]
        focks.append(lax.ppermute(fock_blocks, FRAG, moves))
    table = exchange(table, FRAG)
    focks = [fock.reshape(FRAG_DEV, NB, NB) for fock in focks]
    cross = coupling.reshape(DIM_DEV, NB, NB)
    sent, energies = solve_dimers(dimer_pairs, table, focks, cross)
    arrived = exchange(sent.reshape(N_TEAM, 32, 128), TEAM)
    own, next_1, next_2, energy = sort_blocks(arrived)
    from_1 = lax.ppermute(next_1, PAIR, [(index, index + 1) for index in range(N_PAIR - 1)])
    from_2 = lax.ppermute(next_2, PAIR, [(index, index + 2) for index in range(N_PAIR - 2)])
    energy = lax.ppermute(energy, GRP_FRAG, energy_moves())
    arrived = exchange(join_blocks(own, from_1, from_2, energy), TEAM)
    correction, total = unpack_blocks(arrived, density)
    return correction, energies[0, :DIM_DEV], total.reshape(())


def solution(mesh):
    finer = Mesh(
        mesh.devices.reshape(2, 4, 2, 8, 2), ("grp_0", "grp_1", "frag_0", "frag_1", "frag_2")
    )
    return jax.shard_map(
        per_device,
        mesh=finer,
        in_specs=(
            P(FRAG, None),
            P(FRAG, None),
            P(GRP_FRAG, None),
            P(GRP_FRAG, None),
            P(FRAG),
            P(FRAG),
            P(None, FRAG),
        ),
        out_specs=(P(FRAG, None), P(GRP_FRAG), P()),
        check_vma=False,
    )
```

```python
import jax
import jax.numpy as jnp
from jax import lax
from jax.experimental import pallas as pl
from jax.experimental.pallas import tpu as pltpu
from jax.sharding import Mesh
from jax.sharding import PartitionSpec as P

NB = 96
NA = 16
REACH = 3
PURIF = 12
UNROLL = 6
FRAG_DEV = 8
DIM_DEV = 4
FLAT = NB * NB
FRAG = ("frag_0", "frag_1", "frag_2")
PAIR = ("frag_0", "frag_1")
GRP_FRAG = ("grp_0", "grp_1", "frag_0", "frag_1", "frag_2")
TEAM = ("grp_0", "grp_1", "frag_2")
N_FRAG = 32
N_PAIR = 16
N_TEAM = 16
N_GRP = 8
F32 = jnp.float32
BF16 = jnp.bfloat16
VMEM = pltpu.VMEM
SMEM = pltpu.SMEM

ID_LANE = 96
ONE_LANE = 97
ENERGY_LANE = 98
SUM_LANE = 99


def iota(shape, dim):
    return lax.broadcasted_iota(jnp.int32, shape, dim)


def exchange(value, axis):
    return lax.all_to_all(value, axis, split_axis=0, concat_axis=0, tiled=True)


def dot32(left, right):
    return jnp.dot(left, right, preferred_element_type=F32)


def halves(value):
    high = value.astype(BF16)
    return high, (value - high.astype(F32)).astype(BF16)


def table_kernel(counts, dens, fock, nuclear, coords, table):
    lane = iota((1, 128), 1)
    trace_sum = jnp.zeros((FRAG_DEV, 128), F32)
    diagonal = jnp.zeros((FRAG_DEV, 128), F32)
    for chunk in range(FLAT // 128):
        here = slice(chunk * 128, (chunk + 1) * 128)
        block = dens[:, here].astype(F32)
        trace_sum += block * fock[:, here].astype(F32)
        first = (-chunk * 128) % (NB + 1)
        on_diagonal = jnp.logical_or(lane == first, lane == first + NB + 1)
        diagonal += jnp.where(on_diagonal, block, 0.0)
    fragment = lane // NA
    atom = (lane % NA).astype(F32)
    count = jnp.zeros((1, 128), F32)
    for index in range(FRAG_DEV):
        count = jnp.where(fragment == index, counts[index].astype(F32), count)
    basis = (iota((128, 128), 0) * 33) % 128
    scaled = basis.astype(F32) * count
    inside = jnp.logical_and(atom * NB <= scaled, scaled < (atom + 1.0) * NB)
    owner = jnp.where(jnp.logical_and(inside, basis < NB), 1.0, 0.0).astype(BF16)
    spread = dot32(diagonal.astype(BF16), owner)
    own_lane = iota((FRAG_DEV, 128), 0) == fragment
    population = jnp.sum(jnp.where(own_lane, spread, 0.0), axis=0, keepdims=True)
    traces = jnp.sum(trace_sum, axis=1, keepdims=True)
    at_first = jnp.logical_and(own_lane, lane % NA == 0)
    trace_row = jnp.sum(jnp.where(at_first, traces, 0.0), axis=0, keepdims=True)
    live = jnp.where(atom < count, 1.0, 0.0)
    charge = live * nuclear[...] - 2.0 * population
    row = iota((8, 128), 0)
    rows = [charge, coords[0:1, :], coords[1:2, :], coords[2:3, :], count, population, trace_row]
    value = jnp.zeros((8, 128), F32)
    for index, content in enumerate(rows):
        value = jnp.where(row == index, content, value)
    for peer in range(N_FRAG):
        table[peer] = value


def atom_table(density, fock_blocks, nuclear_charge, atom_counts, coords):
    return pl.pallas_call(
        table_kernel,
        out_shape=jax.ShapeDtypeStruct((N_FRAG, 8, 128), F32),
        in_specs=[pl.BlockSpec(memory_space=SMEM)] + [pl.BlockSpec(memory_space=VMEM)] * 4,
        out_specs=pl.BlockSpec(memory_space=VMEM),
        name="atom_table",
    )(atom_counts, density, fock_blocks, nuclear_charge.reshape(1, 128), coords)


def unflatten(flat, matrices):
    count = flat.shape[0]
    lane = iota((count, 128), 1)
    for quad in range(NB // 4):
        tiles = []
        for tile in range(3 * quad, 3 * quad + 3):
            tiles.append(flat[:, tile * 128 : (tile + 1) * 128].astype(F32))
        row_1 = jnp.where(lane < 96, tiles[1], tiles[0])
        row_2 = jnp.where(lane < 64, tiles[2], tiles[1])
        rows = [
            tiles[0],
            pltpu.roll(row_1, 32, 1),
            pltpu.roll(row_2, 64, 1),
            pltpu.roll(tiles[2], 96, 1),
        ]
        for offset, row in enumerate(rows):
            start = (4 * quad + offset) * 8
            matrices[start : start + count, :] = jnp.where(lane < NB, row, 0.0)


def prepare_kernel(pairs, table, fock, coupling, fixed, starts, columns, masked, fock_rows, cross_rows):
    unflatten(fock, fock_rows)
    unflatten(coupling, cross_rows)
    base = (pairs[0, 0] // FRAG_DEV) * FRAG_DEV
    lane = iota((NA, 128), 1)
    atom = iota((NA, 128), 0).astype(F32)

    source = iota((N_FRAG, 128), 0) * FRAG_DEV + iota((N_FRAG, 128), 1) // NA
    charges = table[:, 0, :]
    for dimer in range(DIM_DEV):
        hidden = jnp.logical_or(source == pairs[dimer, 0], source == pairs[dimer, 1])
        masked[dimer] = jnp.where(hidden, 0.0, charges)
        for side in range(2):
            fragment = pairs[dimer, side]
            columns[2 * dimer + side] = table[fragment // FRAG_DEV].T

    small_eye = iota((NB, 128), 0) == iota((NB, 128), 1)
    for dimer in range(DIM_DEV):
        own, places = [], []
        for side in range(2):
            local = pl.multiple_of((pairs[dimer, side] % FRAG_DEV) * NA, NA)
            mine = columns[2 * dimer + side, pl.ds(local, NA), :]
            own.append(mine)
            places.append([jnp.broadcast_to(mine[:, k : k + 1], (NA, 128)) for k in (1, 2, 3)])

        def gather(step, sums, dimer=dimer, places=places):
            sums = list(sums)
            for inner in range(4):
                block = step * 4 + inner
                weight = masked[dimer, pl.ds(block, 1), :]
                spot = [table[block, k : k + 1, :] for k in (1, 2, 3)]
                for side in range(2):
                    delta = [place - here for place, here in zip(places[side], spot)]
                    distance = delta[0] * delta[0] + delta[1] * delta[1] + delta[2] * delta[2]
                    sums[side] += weight * lax.rsqrt(distance + 1.0)
            return tuple(sums)

        zero = jnp.zeros((NA, 128), F32)
        sums = lax.fori_loop(0, N_FRAG // 4, gather, (zero, zero))
        start = jnp.zeros((1, 1), F32)
        for side in range(2):
            potential = jnp.sum(sums[side], axis=1, keepdims=True)
            count, population, trace = (own[side][:, k : k + 1] for k in (4, 5, 6))
            scaled = lane.astype(F32) * count
            inside = jnp.logical_and(atom * NB <= scaled, scaled < (atom + 1.0) * NB)
            inside = jnp.logical_and(inside, lane < NB)
            shift = jnp.sum(jnp.where(inside, potential, 0.0), axis=0, keepdims=True)
            shift = jnp.where(small_eye, shift, 0.0)
            if side == 0:
                held = pairs[dimer, 0] - base
                shift += fock_rows[pl.ds(held, NB, stride=8), :]
            fixed[dimer, side * NB : (side + 1) * NB, side * 128 : (side + 1) * 128] = shift
            start += jnp.sum(potential * population + trace, axis=0, keepdims=True)
        starts[dimer : dimer + 1, :] = jnp.broadcast_to(start, (1, 128))
        cross = cross_rows[pl.ds(dimer, NB, stride=8), :]
        fixed[dimer, :NB, 128:256] = cross
        fixed[dimer, NB:, :128] = jnp.concatenate(
            [cross.T[:NB, :], jnp.zeros((NB, 128 - NB), F32)], axis=1
        )


def prepare_dimers(pairs, table, fock, coupling):
    return pl.pallas_call(
        prepare_kernel,
        out_shape=(
            jax.ShapeDtypeStruct((DIM_DEV, 2 * NB, 256), F32),
            jax.ShapeDtypeStruct((8, 128), F32),
        ),
        in_specs=[pl.BlockSpec(memory_space=SMEM)] + [pl.BlockSpec(memory_space=VMEM)] * 3,
        out_specs=(pl.BlockSpec(memory_space=VMEM),) * 2,
        scratch_shapes=[
            VMEM((2 * DIM_DEV, 128, 8), F32),
            VMEM((DIM_DEV, N_FRAG, 128), F32),
            VMEM((8 * NB, 128), F32),
            VMEM((8 * NB, 128), F32),
        ],
        compiler_params=pltpu.CompilerParams(vmem_limit_bytes=8 << 20),
        name="prepare_dimers",
    )(pairs, table, fock, coupling)


def solve_kernel(
    pairs, fixed, starts, fock_0, fock_1, fock_2, fock_3, sent, energies,
    fock_rows, shifted, state, high, low, square_high, square_low,
):
    for far, fock in enumerate((fock_0, fock_1, fock_2, fock_3)):
        unflatten(fock, fock_rows.at[far])
    base = (pairs[0, 0] // FRAG_DEV) * FRAG_DEV
    pair_base = (base // NA) * NA
    for buffer in (high, low, square_high, square_low):
        for dimer in range(DIM_DEV):
            buffer[dimer, NB:128, :] = jnp.zeros((128 - NB, 256), BF16)
            buffer[dimer, 128 + NB :, :] = jnp.zeros((128 - NB, 256), BF16)

    rows, cols = iota((2 * NB, 256), 0), iota((2 * NB, 256), 1)
    eye = cols == jnp.where(rows < NB, rows, rows + (128 - NB))
    centres = []
    for dimer in range(DIM_DEV):
        held = pairs[dimer, 1] - base
        part = fock_rows[held // FRAG_DEV, pl.ds(held % FRAG_DEV, NB, stride=8), :]
        shifted[dimer, :NB, :] = fixed[dimer, :NB, :]
        shifted[dimer, NB:, :128] = fixed[dimer, NB:, :128]
        shifted[dimer, NB:, 128:] = fixed[dimer, NB:, 128:] + part
        fock = shifted[dimer]
        trace = jnp.sum(jnp.where(eye, fock, 0.0), axis=(0, 1), keepdims=True)
        centre = trace / (2.0 * NB)
        fock = jnp.where(eye, fock - centre, fock)
        width = jnp.max(jnp.sum(jnp.abs(fock), axis=1, keepdims=True), axis=0, keepdims=True) + 1e-06
        shifted[dimer] = fock
        start = fock / width
        state[dimer] = start
        keep(high, low, dimer, start)
        centres.append(centre)

    def purify(step, carry):
        for dimer in range(DIM_DEV):
            square = product(high, low, dimer, high, low)
            keep(square_high, square_low, dimer, square)
        for dimer in range(DIM_DEV):
            cube = product(high, low, dimer, square_high, square_low)
            later = 1.5 * state[dimer] - 0.5 * cube
            state[dimer] = later
            keep(high, low, dimer, later)
        return carry

    lax.fori_loop(0, PURIF, purify, 0, unroll=UNROLL)

    lane_16 = iota((16, 128), 1)
    for dimer in range(DIM_DEV):
        final = state[dimer]
        overlap = jnp.sum(final * shifted[dimer], axis=(0, 1), keepdims=True)
        trace = jnp.sum(jnp.where(eye, final, 0.0), axis=(0, 1), keepdims=True)
        centre = centres[dimer]
        energy = 0.5 * (2.0 * NB * centre - overlap - centre * trace) - starts[dimer : dimer + 1, 0:1]
        energies[dimer] = jnp.sum(energy)
        for side in range(2):
            slot = side * DIM_DEV + dimer
            block = final[side * NB : (side + 1) * NB, side * 128 : (side + 1) * 128]
            corner = pltpu.roll(block[64:96, :], 32, 1)
            target = (pairs[dimer, side] - pair_base).astype(F32)
            beside = jnp.where(lane_16 == ID_LANE, target, 0.0)
            beside = jnp.where(lane_16 == ONE_LANE, 1.0, beside)
            if side == 0:
                beside = jnp.where(lane_16 == ENERGY_LANE, energy, beside)
            for part in range(4):
                piece = block[16 * part : 16 * (part + 1), :]
                other = corner[16 * part : 16 * (part + 1), :] if part < 2 else beside
                piece = jnp.where(lane_16 < NB, piece, other)
                sent[pl.ds(part * 8 + slot, 16, stride=32), :] = piece


def keep(high, low, dimer, value):
    upper, lower = halves(value)
    for buffer, part in ((high, upper), (low, lower)):
        buffer[dimer, :NB, :] = part[:NB]
        buffer[dimer, 128 : 128 + NB, :] = part[NB:]


def product(high, low, dimer, right_high, right_low):
    upper = [high[dimer, :NB, :], high[dimer, 128 : 128 + NB, :]]
    lower = [low[dimer, :NB, :], low[dimer, 128 : 128 + NB, :]]
    both = dot32(jnp.concatenate(upper + lower, axis=0), right_high[dimer])
    cross = dot32(jnp.concatenate(upper, axis=0), right_low[dimer])
    return both[: 2 * NB] + (both[2 * NB :] + cross)


def solve_dimers(pairs, fixed, starts, focks):
    matrix = (DIM_DEV, 2 * NB, 256)
    split = (DIM_DEV, 256, 256)
    return pl.pallas_call(
        solve_kernel,
        out_shape=(
            jax.ShapeDtypeStruct((N_TEAM * 32, 128), F32),
            jax.ShapeDtypeStruct((DIM_DEV,), F32),
        ),
        in_specs=[pl.BlockSpec(memory_space=SMEM)] + [pl.BlockSpec(memory_space=VMEM)] * 6,
        out_specs=(pl.BlockSpec(memory_space=VMEM), pl.BlockSpec(memory_space=SMEM)),
        scratch_shapes=[
            VMEM((REACH + 1, 8 * NB, 128), F32),
            VMEM(matrix, F32),
            VMEM(matrix, F32),
            VMEM(split, BF16),
            VMEM(split, BF16),
            VMEM(split, BF16),
            VMEM(split, BF16),
        ],
        compiler_params=pltpu.CompilerParams(vmem_limit_bytes=20 << 20),
        name="solve_dimers",
    )(pairs, fixed, starts, *focks)


def sort_kernel(arrived, own, next_1, next_2, energy):
    parts = [
        arrived[:, part * 8 : (part + 1) * 8, :].reshape(N_TEAM * 8, 128) for part in range(4)
    ]
    target = parts[2][:, ID_LANE : ID_LANE + 1].astype(jnp.int32)
    chosen = jnp.where(iota((128, 64), 1) == target, 1.0, 0.0).astype(BF16)
    value = jnp.concatenate(parts, axis=1)
    upper = value.astype(BF16)
    rest = value - upper.astype(F32)
    middle = rest.astype(BF16)
    lower = (rest - middle.astype(F32)).astype(BF16)
    total = jnp.zeros((64, 512), F32)
    for piece in (lower, middle, upper):
        total += lax.dot_general(
            chosen, piece, (((0,), (0,)), ((), ())), preferred_element_type=F32
        )
    own[...] = total[:16]
    next_1[...] = total[16:32].astype(BF16)
    next_2[...] = total[32:48].astype(BF16)
    summed = jnp.sum(parts[2], axis=0, keepdims=True)
    energy[...] = jnp.broadcast_to(summed, (8, 128))


def sort_blocks(arrived):
    return pl.pallas_call(
        sort_kernel,
        out_shape=(
            jax.ShapeDtypeStruct((16, 512), F32),
            jax.ShapeDtypeStruct((16, 512), BF16),
            jax.ShapeDtypeStruct((16, 512), BF16),
            jax.ShapeDtypeStruct((8, 128), F32),
        ),
        in_specs=[pl.BlockSpec(memory_space=VMEM)],
        out_specs=(pl.BlockSpec(memory_space=VMEM),) * 4,
        compiler_params=pltpu.CompilerParams(vmem_limit_bytes=4 << 20),
        name="sort_blocks",
    )(arrived)


def join_kernel(own, from_1, from_2, energy, sent):
    total = own[...] + from_1[...].astype(F32) + from_2[...].astype(F32)
    lane = iota((8, 128), 1)
    mine = jnp.broadcast_to(energy[0:1, ENERGY_LANE : ENERGY_LANE + 1], (8, 128))
    for core in range(2):
        for part in range(4):
            rows = total[core * 8 : core * 8 + 8, part * 128 : (part + 1) * 128]
            if part == 2:
                rows = jnp.where(lane == SUM_LANE, mine, rows)
            for group in range(N_GRP):
                sent[2 * group + core, part * 8 : (part + 1) * 8, :] = rows


def join_blocks(own, from_1, from_2, energy):
    return pl.pallas_call(
        join_kernel,
        out_shape=jax.ShapeDtypeStruct((N_TEAM, 32, 128), F32),
        in_specs=[pl.BlockSpec(memory_space=VMEM)] * 4,
        out_specs=pl.BlockSpec(memory_space=VMEM),
        compiler_params=pltpu.CompilerParams(vmem_limit_bytes=4 << 20),
        name="join_blocks",
    )(own, from_1, from_2, energy)


def unpack_kernel(arrived, dens, out, total, turned):
    for fragment in range(FRAG_DEV):
        upper = jnp.concatenate(
            [
                arrived[pl.ds(part * 8 + fragment, 16, stride=32), :]
                for part in range(4)
            ],
            axis=0,
        )
        turned[pl.ds(fragment, 32, stride=8), :] = jnp.concatenate(
            [upper.T[64:96, :], jnp.zeros((32, 64), F32)], axis=1
        )
    lane = iota((8, 128), 1)
    number = arrived[16:24, ONE_LANE : ONE_LANE + 1]
    number = jnp.broadcast_to(number, (8, 128))
    half_number = 0.5 * number

    def packed(row):
        start = (row % 16) * 32 + (row // 16) * 8
        return arrived[start : start + 8, :]

    def matrix_row(row):
        if row < 64:
            return packed(row)
        left = turned[(row - 64) * 8 : (row - 64) * 8 + 8, :]
        right = pltpu.roll(packed(row - 64), 96, 1)
        return jnp.where(lane < 64, left, right)

    def finish(tile, value):
        here = slice(tile * 128, (tile + 1) * 128)
        first = (-tile * 128) % (NB + 1)
        on_diagonal = jnp.logical_or(lane == first, lane == first + NB + 1)
        value = -0.5 * value - number * dens[:, here].astype(F32)
        out[:, here] = value + jnp.where(on_diagonal, half_number, 0.0)

    for quad in range(NB // 4):
        row_0 = matrix_row(4 * quad)
        row_1 = pltpu.roll(matrix_row(4 * quad + 1), 96, 1)
        row_2 = pltpu.roll(matrix_row(4 * quad + 2), 64, 1)
        row_3 = pltpu.roll(matrix_row(4 * quad + 3), 32, 1)
        finish(3 * quad, jnp.where(lane < 96, row_0, row_1))
        finish(3 * quad + 1, jnp.where(lane < 64, row_1, row_2))
        finish(3 * quad + 2, jnp.where(lane < 32, row_2, row_3))

    energy = jnp.zeros((1, 128), F32)
    for member in range(N_TEAM):
        energy += arrived[member * 32 + 16 : member * 32 + 17, :]
    total[...] = energy[:, SUM_LANE : SUM_LANE + 1]


def unpack_blocks(arrived, density):
    return pl.pallas_call(
        unpack_kernel,
        out_shape=(
            jax.ShapeDtypeStruct((FRAG_DEV, FLAT), F32),
            jax.ShapeDtypeStruct((1, 1), F32),
        ),
        in_specs=[pl.BlockSpec(memory_space=VMEM)] * 2,
        out_specs=(pl.BlockSpec(memory_space=VMEM),) * 2,
        scratch_shapes=[VMEM((256, 128), F32)],
        compiler_params=pltpu.CompilerParams(vmem_limit_bytes=4 << 20),
        name="unpack_blocks",
    )(arrived.reshape(N_TEAM * 32, 128), density)


def energy_moves():
    moves = []
    for group in range(N_GRP):
        for pair in range(N_PAIR):
            for core in range(2):
                source = group * N_FRAG + pair * 2 + core
                away = (pair + 2 * group + core) % N_PAIR
                moves.append((source, group * N_FRAG + away * 2 + core))
    return moves


def per_device(density, fock_blocks, coupling, dimer_pairs, atom_counts, nuclear_charge, coords):
    table = atom_table(density, fock_blocks, nuclear_charge, atom_counts, coords)
    focks = [fock_blocks]
    for distance in range(1, REACH + 1):
        moves = [(index + distance, index) for index in range(N_FRAG - distance)]
        focks.append(lax.ppermute(fock_blocks, FRAG, moves))
    table = exchange(table, FRAG)
    fixed, starts = prepare_dimers(dimer_pairs, table, fock_blocks, coupling)
    sent, energies = solve_dimers(dimer_pairs, fixed, starts, focks)
    arrived = exchange(sent.reshape(N_TEAM, 32, 128), TEAM)
    own, next_1, next_2, energy = sort_blocks(arrived)
    from_1 = lax.ppermute(next_1, PAIR, [(index, index + 1) for index in range(N_PAIR - 1)])
    from_2 = lax.ppermute(next_2, PAIR, [(index, index + 2) for index in range(N_PAIR - 2)])
    energy = lax.ppermute(energy, GRP_FRAG, energy_moves())
    arrived = exchange(join_blocks(own, from_1, from_2, energy), TEAM)
    correction, total = unpack_blocks(arrived, density)
    return correction, energies, total.reshape(())


def solution(mesh):
    finer = Mesh(
        mesh.devices.reshape(2, 4, 2, 8, 2), ("grp_0", "grp_1", "frag_0", "frag_1", "frag_2")
    )
    return jax.shard_map(
        per_device,
        mesh=finer,
        in_specs=(
            P(FRAG, None),
            P(FRAG, None),
            P(GRP_FRAG, None),
            P(GRP_FRAG, None),
            P(FRAG),
            P(FRAG),
            P(None, FRAG),
        ),
        out_specs=(P(FRAG, None), P(GRP_FRAG), P()),
        check_vma=False,
    )
```

```python
import jax
import jax.numpy as jnp
from jax import lax
from jax.experimental import pallas as pl
from jax.experimental.pallas import tpu as pltpu
from jax.sharding import Mesh
from jax.sharding import PartitionSpec as P

NB = 96
NA = 16
REACH = 3
PURIF = 12
UNROLL = 6
FRAG_DEV = 8
DIM_DEV = 4
FLAT = NB * NB
FRAG = ("frag_0", "frag_1", "frag_2")
PAIR = ("frag_0", "frag_1")
GRP_FRAG = ("grp_0", "grp_1", "frag_0", "frag_1", "frag_2")
TEAM = ("grp_0", "grp_1", "frag_2")
N_FRAG = 32
N_PAIR = 16
N_TEAM = 16
N_GRP = 8
F32 = jnp.float32
BF16 = jnp.bfloat16
VMEM = pltpu.VMEM
SMEM = pltpu.SMEM

ID_LANE = 96
ONE_LANE = 97
ENERGY_LANE = 98
SUM_LANE = 99


def iota(shape, dim):
    return lax.broadcasted_iota(jnp.int32, shape, dim)


def exchange(value, axis):
    return lax.all_to_all(value, axis, split_axis=0, concat_axis=0, tiled=True)


def dot32(left, right):
    return jnp.dot(left, right, preferred_element_type=F32)


def halves(value):
    high = value.astype(BF16)
    return high, (value - high.astype(F32)).astype(BF16)


def table_kernel(counts, dens, fock, nuclear, coords, table, packed, matrices):
    lane = iota((1, 128), 1)
    trace_sum = jnp.zeros((FRAG_DEV, 128), F32)
    diagonal = jnp.zeros((FRAG_DEV, 128), F32)
    for chunk in range(FLAT // 128):
        here = slice(chunk * 128, (chunk + 1) * 128)
        block = dens[:, here].astype(F32)
        trace_sum += block * fock[:, here].astype(F32)
        first = (-chunk * 128) % (NB + 1)
        on_diagonal = jnp.logical_or(lane == first, lane == first + NB + 1)
        diagonal += jnp.where(on_diagonal, block, 0.0)
    fragment = lane // NA
    atom = (lane % NA).astype(F32)
    count = jnp.zeros((1, 128), F32)
    for index in range(FRAG_DEV):
        count = jnp.where(fragment == index, counts[index].astype(F32), count)
    basis = (iota((128, 128), 0) * 33) % 128
    scaled = basis.astype(F32) * count
    inside = jnp.logical_and(atom * NB <= scaled, scaled < (atom + 1.0) * NB)
    owner = jnp.where(jnp.logical_and(inside, basis < NB), 1.0, 0.0).astype(BF16)
    spread = dot32(diagonal.astype(BF16), owner)
    own_lane = iota((FRAG_DEV, 128), 0) == fragment
    population = jnp.sum(jnp.where(own_lane, spread, 0.0), axis=0, keepdims=True)
    traces = jnp.sum(trace_sum, axis=1, keepdims=True)
    at_first = jnp.logical_and(own_lane, lane % NA == 0)
    trace_row = jnp.sum(jnp.where(at_first, traces, 0.0), axis=0, keepdims=True)
    live = jnp.where(atom < count, 1.0, 0.0)
    charge = live * nuclear[...] - 2.0 * population
    row = iota((8, 128), 0)
    rows = [charge, coords[0:1, :], coords[1:2, :], coords[2:3, :], count, population, trace_row]
    value = jnp.zeros((8, 128), F32)
    for index, content in enumerate(rows):
        value = jnp.where(row == index, content, value)
    for peer in range(N_FRAG):
        table[peer] = value
    unflatten(fock, matrices)
    pack_rows(matrices, packed)


def pack_rows(matrices, packed):
    lane = iota((8, 128), 1)

    def row(index):
        return matrices[8 * index : 8 * index + 8, :]

    rows = [
        jnp.where(lane < NB, row(index), pltpu.roll(row(64 + index), 32, 1)) for index in range(32)
    ]
    for index in range(16):
        left, right = pltpu.roll(row(32 + index), 96, 1), pltpu.roll(row(48 + index), 32, 1)
        rows.append(jnp.where(lane < 64, left, right))
    for index in range(0, 48, 2):
        both = jnp.concatenate(rows[index : index + 2], axis=0)
        packed[8 * index : 8 * index + 16, :] = both.astype(BF16)


def unpacked(rows):
    lane = iota((32, 128), 1)
    top, middle = rows[:32, :], rows[32:, :]
    turned = jnp.concatenate([rows, jnp.zeros((80, 128), F32)], axis=0).T
    first = jnp.where(lane < NB, top, 0.0)
    beside = jnp.concatenate([pltpu.roll(middle, 32, 1), pltpu.roll(middle, 96, 1)], axis=0)
    second = jnp.where(lane < 32, turned[32:64, :], jnp.where(lane < NB, beside, 0.0))
    third = jnp.where(lane < NB, pltpu.roll(top, 96, 1), 0.0)
    third = jnp.where(lane < 64, pltpu.roll(turned[96:128, :], 16, 1), third)
    third = jnp.where(lane < 48, turned[32:64, :], third)
    third = jnp.where(lane < 32, turned[64:96, :], third)
    return jnp.concatenate([first, second, third], axis=0)


def atom_table(density, fock_blocks, nuclear_charge, atom_counts, coords):
    return pl.pallas_call(
        table_kernel,
        out_shape=(
            jax.ShapeDtypeStruct((N_FRAG, 8, 128), F32),
            jax.ShapeDtypeStruct((48 * FRAG_DEV, 128), BF16),
        ),
        in_specs=[pl.BlockSpec(memory_space=SMEM)] + [pl.BlockSpec(memory_space=VMEM)] * 4,
        out_specs=(pl.BlockSpec(memory_space=VMEM),) * 2,
        scratch_shapes=[VMEM((8 * NB, 128), F32)],
        name="atom_table",
    )(atom_counts, density, fock_blocks, nuclear_charge.reshape(1, 128), coords)


def unflatten(flat, matrices):
    count = flat.shape[0]
    lane = iota((count, 128), 1)
    for quad in range(NB // 4):
        tiles = []
        for tile in range(3 * quad, 3 * quad + 3):
            tiles.append(flat[:, tile * 128 : (tile + 1) * 128].astype(F32))
        row_1 = jnp.where(lane < 96, tiles[1], tiles[0])
        row_2 = jnp.where(lane < 64, tiles[2], tiles[1])
        rows = [
            tiles[0],
            pltpu.roll(row_1, 32, 1),
            pltpu.roll(row_2, 64, 1),
            pltpu.roll(tiles[2], 96, 1),
        ]
        for offset, row in enumerate(rows):
            start = (4 * quad + offset) * 8
            matrices[start : start + count, :] = jnp.where(lane < NB, row, 0.0)


def prepare_kernel(pairs, table, fock, coupling, fixed, starts, columns, masked, fock_rows, cross_rows):
    unflatten(fock, fock_rows)
    unflatten(coupling, cross_rows)
    base = (pairs[0, 0] // FRAG_DEV) * FRAG_DEV
    lane = iota((NA, 128), 1)
    atom = iota((NA, 128), 0).astype(F32)

    source = iota((N_FRAG, 128), 0) * FRAG_DEV + iota((N_FRAG, 128), 1) // NA
    charges = table[:, 0, :]
    for dimer in range(DIM_DEV):
        hidden = jnp.logical_or(source == pairs[dimer, 0], source == pairs[dimer, 1])
        masked[dimer] = jnp.where(hidden, 0.0, charges)
        for side in range(2):
            fragment = pairs[dimer, side]
            columns[2 * dimer + side] = table[fragment // FRAG_DEV].T

    small_eye = iota((NB, 128), 0) == iota((NB, 128), 1)
    for dimer in range(DIM_DEV):
        own, places = [], []
        for side in range(2):
            local = pl.multiple_of((pairs[dimer, side] % FRAG_DEV) * NA, NA)
            mine = columns[2 * dimer + side, pl.ds(local, NA), :]
            own.append(mine)
            places.append([jnp.broadcast_to(mine[:, k : k + 1], (NA, 128)) for k in (1, 2, 3)])

        def gather(step, sums, dimer=dimer, places=places):
            sums = list(sums)
            for inner in range(4):
                block = step * 4 + inner
                weight = masked[dimer, pl.ds(block, 1), :]
                spot = [table[block, k : k + 1, :] for k in (1, 2, 3)]
                for side in range(2):
                    delta = [place - here for place, here in zip(places[side], spot)]
                    distance = delta[0] * delta[0] + delta[1] * delta[1] + delta[2] * delta[2]
                    sums[side] += weight * lax.rsqrt(distance + 1.0)
            return tuple(sums)

        zero = jnp.zeros((NA, 128), F32)
        sums = lax.fori_loop(0, N_FRAG // 4, gather, (zero, zero))
        start = jnp.zeros((1, 1), F32)
        for side in range(2):
            potential = jnp.sum(sums[side], axis=1, keepdims=True)
            count, population, trace = (own[side][:, k : k + 1] for k in (4, 5, 6))
            scaled = lane.astype(F32) * count
            inside = jnp.logical_and(atom * NB <= scaled, scaled < (atom + 1.0) * NB)
            inside = jnp.logical_and(inside, lane < NB)
            shift = jnp.sum(jnp.where(inside, potential, 0.0), axis=0, keepdims=True)
            shift = jnp.where(small_eye, shift, 0.0)
            if side == 0:
                held = pairs[dimer, 0] - base
                shift += fock_rows[pl.ds(held, NB, stride=8), :]
            fixed[dimer, side * NB : (side + 1) * NB, side * 128 : (side + 1) * 128] = shift
            start += jnp.sum(potential * population + trace, axis=0, keepdims=True)
        starts[dimer : dimer + 1, :] = jnp.broadcast_to(start, (1, 128))
        cross = cross_rows[pl.ds(dimer, NB, stride=8), :]
        fixed[dimer, :NB, 128:256] = cross
        fixed[dimer, NB:, :128] = jnp.concatenate(
            [cross.T[:NB, :], jnp.zeros((NB, 128 - NB), F32)], axis=1
        )


def prepare_dimers(pairs, table, fock, coupling):
    return pl.pallas_call(
        prepare_kernel,
        out_shape=(
            jax.ShapeDtypeStruct((DIM_DEV, 2 * NB, 256), F32),
            jax.ShapeDtypeStruct((8, 128), F32),
        ),
        in_specs=[pl.BlockSpec(memory_space=SMEM)] + [pl.BlockSpec(memory_space=VMEM)] * 3,
        out_specs=(pl.BlockSpec(memory_space=VMEM),) * 2,
        scratch_shapes=[
            VMEM((2 * DIM_DEV, 128, 8), F32),
            VMEM((DIM_DEV, N_FRAG, 128), F32),
            VMEM((8 * NB, 128), F32),
            VMEM((8 * NB, 128), F32),
        ],
        compiler_params=pltpu.CompilerParams(vmem_limit_bytes=8 << 20),
        name="prepare_dimers",
    )(pairs, table, fock, coupling)


def solve_kernel(
    pairs, fixed, starts, fock_0, fock_1, fock_2, fock_3, sent, energies,
    fock_rows, shifted, state, high, low, square_high, square_low,
):
    for far, fock in enumerate((fock_0, fock_1, fock_2, fock_3)):
        fock_rows[far] = fock[...].astype(F32)
    base = (pairs[0, 0] // FRAG_DEV) * FRAG_DEV
    pair_base = (base // NA) * NA
    for buffer in (high, low, square_high, square_low):
        for dimer in range(DIM_DEV):
            buffer[dimer, NB:128, :] = jnp.zeros((128 - NB, 256), BF16)
            buffer[dimer, 128 + NB :, :] = jnp.zeros((128 - NB, 256), BF16)

    rows, cols = iota((2 * NB, 256), 0), iota((2 * NB, 256), 1)
    eye = cols == jnp.where(rows < NB, rows, rows + (128 - NB))
    centres = []
    for dimer in range(DIM_DEV):
        held = pairs[dimer, 1] - base
        part = unpacked(fock_rows[held // FRAG_DEV, pl.ds(held % FRAG_DEV, 48, stride=8), :])
        shifted[dimer, :NB, :] = fixed[dimer, :NB, :]
        shifted[dimer, NB:, :128] = fixed[dimer, NB:, :128]
        shifted[dimer, NB:, 128:] = fixed[dimer, NB:, 128:] + part
        fock = shifted[dimer]
        trace = jnp.sum(jnp.where(eye, fock, 0.0), axis=(0, 1), keepdims=True)
        centre = trace / (2.0 * NB)
        fock = jnp.where(eye, fock - centre, fock)
        width = jnp.max(jnp.sum(jnp.abs(fock), axis=1, keepdims=True), axis=0, keepdims=True) + 1e-06
        shifted[dimer] = fock
        start = fock / width
        state[dimer] = start
        keep(high, low, dimer, start)
        centres.append(centre)

    def purify(step, carry):
        for dimer in range(DIM_DEV):
            square = product(high, low, dimer, high, low)
            keep(square_high, square_low, dimer, square)
        for dimer in range(DIM_DEV):
            cube = product(high, low, dimer, square_high, square_low)
            later = 1.5 * state[dimer] - 0.5 * cube
            state[dimer] = later
            keep(high, low, dimer, later)
        return carry

    lax.fori_loop(0, PURIF, purify, 0, unroll=UNROLL)

    lane_16 = iota((16, 128), 1)
    for dimer in range(DIM_DEV):
        final = state[dimer]
        overlap = jnp.sum(final * shifted[dimer], axis=(0, 1), keepdims=True)
        trace = jnp.sum(jnp.where(eye, final, 0.0), axis=(0, 1), keepdims=True)
        centre = centres[dimer]
        energy = 0.5 * (2.0 * NB * centre - overlap - centre * trace) - starts[dimer : dimer + 1, 0:1]
        energies[dimer] = jnp.sum(energy)
        for side in range(2):
            slot = side * DIM_DEV + dimer
            block = final[side * NB : (side + 1) * NB, side * 128 : (side + 1) * 128]
            corner = pltpu.roll(block[64:96, :], 32, 1)
            target = (pairs[dimer, side] - pair_base).astype(F32)
            beside = jnp.where(lane_16 == ID_LANE, target, 0.0)
            beside = jnp.where(lane_16 == ONE_LANE, 1.0, beside)
            if side == 0:
                beside = jnp.where(lane_16 == ENERGY_LANE, energy, beside)
            for part in range(4):
                piece = block[16 * part : 16 * (part + 1), :]
                other = corner[16 * part : 16 * (part + 1), :] if part < 2 else beside
                piece = jnp.where(lane_16 < NB, piece, other)
                sent[pl.ds(part * 8 + slot, 16, stride=32), :] = piece


def keep(high, low, dimer, value):
    upper, lower = halves(value)
    for buffer, part in ((high, upper), (low, lower)):
        buffer[dimer, :NB, :] = part[:NB]
        buffer[dimer, 128 : 128 + NB, :] = part[NB:]


def product(high, low, dimer, right_high, right_low):
    upper = [high[dimer, :NB, :], high[dimer, 128 : 128 + NB, :]]
    lower = [low[dimer, :NB, :], low[dimer, 128 : 128 + NB, :]]
    both = dot32(jnp.concatenate(upper + lower, axis=0), right_high[dimer])
    cross = dot32(jnp.concatenate(upper, axis=0), right_low[dimer])
    return both[: 2 * NB] + (both[2 * NB :] + cross)


def solve_dimers(pairs, fixed, starts, focks):
    matrix = (DIM_DEV, 2 * NB, 256)
    split = (DIM_DEV, 256, 256)
    return pl.pallas_call(
        solve_kernel,
        out_shape=(
            jax.ShapeDtypeStruct((N_TEAM * 32, 128), F32),
            jax.ShapeDtypeStruct((DIM_DEV,), F32),
        ),
        in_specs=[pl.BlockSpec(memory_space=SMEM)] + [pl.BlockSpec(memory_space=VMEM)] * 6,
        out_specs=(pl.BlockSpec(memory_space=VMEM), pl.BlockSpec(memory_space=SMEM)),
        scratch_shapes=[
            VMEM((REACH + 1, 48 * FRAG_DEV, 128), F32),
            VMEM(matrix, F32),
            VMEM(matrix, F32),
            VMEM(split, BF16),
            VMEM(split, BF16),
            VMEM(split, BF16),
            VMEM(split, BF16),
        ],
        compiler_params=pltpu.CompilerParams(vmem_limit_bytes=20 << 20),
        name="solve_dimers",
    )(pairs, fixed, starts, *focks)


def sort_kernel(arrived, own, next_1, next_2, energy):
    parts = [
        arrived[:, part * 8 : (part + 1) * 8, :].reshape(N_TEAM * 8, 128) for part in range(4)
    ]
    target = parts[2][:, ID_LANE : ID_LANE + 1].astype(jnp.int32)
    chosen = jnp.where(iota((128, 64), 1) == target, 1.0, 0.0).astype(BF16)
    value = jnp.concatenate(parts, axis=1)
    upper = value.astype(BF16)
    rest = value - upper.astype(F32)
    middle = rest.astype(BF16)
    lower = (rest - middle.astype(F32)).astype(BF16)
    total = jnp.zeros((64, 512), F32)
    for piece in (lower, middle, upper):
        total += lax.dot_general(
            chosen, piece, (((0,), (0,)), ((), ())), preferred_element_type=F32
        )
    own[...] = total[:16]
    next_1[...] = total[16:32].astype(BF16)
    next_2[...] = total[32:48].astype(BF16)
    summed = jnp.sum(parts[2], axis=0, keepdims=True)
    energy[...] = jnp.broadcast_to(summed, (8, 128))


def sort_blocks(arrived):
    return pl.pallas_call(
        sort_kernel,
        out_shape=(
            jax.ShapeDtypeStruct((16, 512), F32),
            jax.ShapeDtypeStruct((16, 512), BF16),
            jax.ShapeDtypeStruct((16, 512), BF16),
            jax.ShapeDtypeStruct((8, 128), F32),
        ),
        in_specs=[pl.BlockSpec(memory_space=VMEM)],
        out_specs=(pl.BlockSpec(memory_space=VMEM),) * 4,
        compiler_params=pltpu.CompilerParams(vmem_limit_bytes=4 << 20),
        name="sort_blocks",
    )(arrived)


def join_kernel(own, from_1, from_2, energy, sent):
    total = own[...] + from_1[...].astype(F32) + from_2[...].astype(F32)
    lane = iota((8, 128), 1)
    mine = jnp.broadcast_to(energy[0:1, ENERGY_LANE : ENERGY_LANE + 1], (8, 128))
    for core in range(2):
        for part in range(4):
            rows = total[core * 8 : core * 8 + 8, part * 128 : (part + 1) * 128]
            if part == 2:
                rows = jnp.where(lane == SUM_LANE, mine, rows)
            for group in range(N_GRP):
                sent[2 * group + core, part * 8 : (part + 1) * 8, :] = rows


def join_blocks(own, from_1, from_2, energy):
    return pl.pallas_call(
        join_kernel,
        out_shape=jax.ShapeDtypeStruct((N_TEAM, 32, 128), F32),
        in_specs=[pl.BlockSpec(memory_space=VMEM)] * 4,
        out_specs=pl.BlockSpec(memory_space=VMEM),
        compiler_params=pltpu.CompilerParams(vmem_limit_bytes=4 << 20),
        name="join_blocks",
    )(own, from_1, from_2, energy)


def unpack_kernel(arrived, dens, out, total, turned):
    for fragment in range(FRAG_DEV):
        upper = jnp.concatenate(
            [
                arrived[pl.ds(part * 8 + fragment, 16, stride=32), :]
                for part in range(4)
            ],
            axis=0,
        )
        turned[pl.ds(fragment, 32, stride=8), :] = jnp.concatenate(
            [upper.T[64:96, :], jnp.zeros((32, 64), F32)], axis=1
        )
    lane = iota((8, 128), 1)
    number = arrived[16:24, ONE_LANE : ONE_LANE + 1]
    number = jnp.broadcast_to(number, (8, 128))
    half_number = 0.5 * number

    def packed(row):
        start = (row % 16) * 32 + (row // 16) * 8
        return arrived[start : start + 8, :]

    def matrix_row(row):
        if row < 64:
            return packed(row)
        left = turned[(row - 64) * 8 : (row - 64) * 8 + 8, :]
        right = pltpu.roll(packed(row - 64), 96, 1)
        return jnp.where(lane < 64, left, right)

    def finish(tile, value):
        here = slice(tile * 128, (tile + 1) * 128)
        first = (-tile * 128) % (NB + 1)
        on_diagonal = jnp.logical_or(lane == first, lane == first + NB + 1)
        value = -0.5 * value - number * dens[:, here].astype(F32)
        out[:, here] = value + jnp.where(on_diagonal, half_number, 0.0)

    for quad in range(NB // 4):
        row_0 = matrix_row(4 * quad)
        row_1 = pltpu.roll(matrix_row(4 * quad + 1), 96, 1)
        row_2 = pltpu.roll(matrix_row(4 * quad + 2), 64, 1)
        row_3 = pltpu.roll(matrix_row(4 * quad + 3), 32, 1)
        finish(3 * quad, jnp.where(lane < 96, row_0, row_1))
        finish(3 * quad + 1, jnp.where(lane < 64, row_1, row_2))
        finish(3 * quad + 2, jnp.where(lane < 32, row_2, row_3))

    energy = jnp.zeros((1, 128), F32)
    for member in range(N_TEAM):
        energy += arrived[member * 32 + 16 : member * 32 + 17, :]
    total[...] = energy[:, SUM_LANE : SUM_LANE + 1]


def unpack_blocks(arrived, density):
    return pl.pallas_call(
        unpack_kernel,
        out_shape=(
            jax.ShapeDtypeStruct((FRAG_DEV, FLAT), F32),
            jax.ShapeDtypeStruct((1, 1), F32),
        ),
        in_specs=[pl.BlockSpec(memory_space=VMEM)] * 2,
        out_specs=(pl.BlockSpec(memory_space=VMEM),) * 2,
        scratch_shapes=[VMEM((256, 128), F32)],
        compiler_params=pltpu.CompilerParams(vmem_limit_bytes=4 << 20),
        name="unpack_blocks",
    )(arrived.reshape(N_TEAM * 32, 128), density)


def energy_moves():
    moves = []
    for group in range(N_GRP):
        for pair in range(N_PAIR):
            for core in range(2):
                source = group * N_FRAG + pair * 2 + core
                away = (pair + 2 * group + core) % N_PAIR
                moves.append((source, group * N_FRAG + away * 2 + core))
    return moves


def per_device(density, fock_blocks, coupling, dimer_pairs, atom_counts, nuclear_charge, coords):
    table, packed = atom_table(density, fock_blocks, nuclear_charge, atom_counts, coords)
    focks = [packed]
    for distance in range(1, REACH + 1):
        moves = [(index + distance, index) for index in range(N_FRAG - distance)]
        focks.append(lax.ppermute(packed, FRAG, moves))
    table = exchange(table, FRAG)
    fixed, starts = prepare_dimers(dimer_pairs, table, fock_blocks, coupling)
    sent, energies = solve_dimers(dimer_pairs, fixed, starts, focks)
    arrived = exchange(sent.reshape(N_TEAM, 32, 128), TEAM)
    own, next_1, next_2, energy = sort_blocks(arrived)
    from_1 = lax.ppermute(next_1, PAIR, [(index, index + 1) for index in range(N_PAIR - 1)])
    from_2 = lax.ppermute(next_2, PAIR, [(index, index + 2) for index in range(N_PAIR - 2)])
    energy = lax.ppermute(energy, GRP_FRAG, energy_moves())
    arrived = exchange(join_blocks(own, from_1, from_2, energy), TEAM)
    correction, total = unpack_blocks(arrived, density)
    return correction, energies, total.reshape(())


def solution(mesh):
    finer = Mesh(
        mesh.devices.reshape(2, 4, 2, 8, 2), ("grp_0", "grp_1", "frag_0", "frag_1", "frag_2")
    )
    return jax.shard_map(
        per_device,
        mesh=finer,
        in_specs=(
            P(FRAG, None),
            P(FRAG, None),
            P(GRP_FRAG, None),
            P(GRP_FRAG, None),
            P(FRAG),
            P(FRAG),
            P(None, FRAG),
        ),
        out_specs=(P(FRAG, None), P(GRP_FRAG), P()),
        check_vma=False,
    )
```

```python
import jax
import jax.numpy as jnp
from jax import lax
from jax.experimental import pallas as pl
from jax.experimental.pallas import tpu as pltpu
from jax.sharding import Mesh
from jax.sharding import PartitionSpec as P

NB = 96
NA = 16
REACH = 3
PURIF = 12
UNROLL = 6
BATCH = 8
FRAG_DEV = 8
DIM_DEV = 4
FLAT = NB * NB
FRAG = ("frag_0", "frag_1", "frag_2")
PAIR = ("frag_0", "frag_1")
GRP_FRAG = ("grp_0", "grp_1", "frag_0", "frag_1", "frag_2")
TEAM = ("grp_0", "grp_1", "frag_2")
N_FRAG = 32
N_PAIR = 16
N_TEAM = 16
N_GRP = 8
F32 = jnp.float32
BF16 = jnp.bfloat16
VMEM = pltpu.VMEM
SMEM = pltpu.SMEM

PARTS = 3
ID_LANE = 64
ONE_LANE = 65
ENERGY_LANE = 66
SUM_LANE = 67


def iota(shape, dim):
    return lax.broadcasted_iota(jnp.int32, shape, dim)


def exchange(value, axis):
    return lax.all_to_all(value, axis, split_axis=0, concat_axis=0, tiled=True)


def dot32(left, right):
    return jnp.dot(left, right, preferred_element_type=F32)


def halves(value):
    high = value.astype(BF16)
    return high, (value - high.astype(F32)).astype(BF16)


def table_kernel(counts, dens, fock, nuclear, coords, table, packed, matrices):
    lane = iota((1, 128), 1)
    trace_sum = jnp.zeros((FRAG_DEV, 128), F32)
    diagonal = jnp.zeros((FRAG_DEV, 128), F32)
    for chunk in range(FLAT // 128):
        here = slice(chunk * 128, (chunk + 1) * 128)
        block = dens[:, here].astype(F32)
        trace_sum += block * fock[:, here].astype(F32)
        first = (-chunk * 128) % (NB + 1)
        on_diagonal = jnp.logical_or(lane == first, lane == first + NB + 1)
        diagonal += jnp.where(on_diagonal, block, 0.0)
    fragment = lane // NA
    atom = (lane % NA).astype(F32)
    count = jnp.zeros((1, 128), F32)
    for index in range(FRAG_DEV):
        count = jnp.where(fragment == index, counts[index].astype(F32), count)
    basis = (iota((128, 128), 0) * 33) % 128
    scaled = basis.astype(F32) * count
    inside = jnp.logical_and(atom * NB <= scaled, scaled < (atom + 1.0) * NB)
    owner = jnp.where(jnp.logical_and(inside, basis < NB), 1.0, 0.0).astype(BF16)
    spread = dot32(diagonal.astype(BF16), owner)
    own_lane = iota((FRAG_DEV, 128), 0) == fragment
    population = jnp.sum(jnp.where(own_lane, spread, 0.0), axis=0, keepdims=True)
    traces = jnp.sum(trace_sum, axis=1, keepdims=True)
    at_first = jnp.logical_and(own_lane, lane % NA == 0)
    trace_row = jnp.sum(jnp.where(at_first, traces, 0.0), axis=0, keepdims=True)
    live = jnp.where(atom < count, 1.0, 0.0)
    charge = live * nuclear[...] - 2.0 * population
    row = iota((8, 128), 0)
    rows = [charge, coords[0:1, :], coords[1:2, :], coords[2:3, :], count, population, trace_row]
    value = jnp.zeros((8, 128), F32)
    for index, content in enumerate(rows):
        value = jnp.where(row == index, content, value)
    for peer in range(N_FRAG):
        table[peer] = value
    unflatten(fock, matrices)
    pack_rows(matrices, packed)


def pack_rows(matrices, packed):
    lane = iota((8, 128), 1)

    def row(index):
        return matrices[8 * index : 8 * index + 8, :]

    rows = [
        jnp.where(lane < NB, row(index), pltpu.roll(row(64 + index), 32, 1)) for index in range(32)
    ]
    for index in range(16):
        left, right = pltpu.roll(row(32 + index), 96, 1), pltpu.roll(row(48 + index), 32, 1)
        rows.append(jnp.where(lane < 64, left, right))
    for index in range(0, 48, 2):
        both = jnp.concatenate(rows[index : index + 2], axis=0)
        packed[8 * index : 8 * index + 16, :] = both.astype(BF16)


def unpacked(rows):
    lane = iota((32, 128), 1)
    top, middle = rows[:32, :], rows[32:, :]
    turned = jnp.concatenate([rows, jnp.zeros((80, 128), F32)], axis=0).T
    first = jnp.where(lane < NB, top, 0.0)
    beside = jnp.concatenate([pltpu.roll(middle, 32, 1), pltpu.roll(middle, 96, 1)], axis=0)
    second = jnp.where(lane < 32, turned[32:64, :], jnp.where(lane < NB, beside, 0.0))
    mirrored = jnp.logical_and(iota((32, 128), 0) >= 16, jnp.logical_and(lane >= 32, lane < 48))
    second = jnp.where(mirrored, turned[:32, :], second)
    third = jnp.where(lane < NB, pltpu.roll(top, 96, 1), 0.0)
    third = jnp.where(lane < 64, pltpu.roll(turned[96:128, :], 16, 1), third)
    third = jnp.where(lane < 48, turned[32:64, :], third)
    third = jnp.where(lane < 32, turned[64:96, :], third)
    return jnp.concatenate([first, second, third], axis=0)


def atom_table(density, fock_blocks, nuclear_charge, atom_counts, coords):
    return pl.pallas_call(
        table_kernel,
        out_shape=(
            jax.ShapeDtypeStruct((N_FRAG, 8, 128), F32),
            jax.ShapeDtypeStruct((48 * FRAG_DEV, 128), BF16),
        ),
        in_specs=[pl.BlockSpec(memory_space=SMEM)] + [pl.BlockSpec(memory_space=VMEM)] * 4,
        out_specs=(pl.BlockSpec(memory_space=VMEM),) * 2,
        scratch_shapes=[VMEM((8 * NB, 128), F32)],
        name="atom_table",
    )(atom_counts, density, fock_blocks, nuclear_charge.reshape(1, 128), coords)


def unflatten(flat, matrices):
    count = flat.shape[0]
    lane = iota((count, 128), 1)
    for quad in range(NB // 4):
        tiles = []
        for tile in range(3 * quad, 3 * quad + 3):
            tiles.append(flat[:, tile * 128 : (tile + 1) * 128].astype(F32))
        row_1 = jnp.where(lane < 96, tiles[1], tiles[0])
        row_2 = jnp.where(lane < 64, tiles[2], tiles[1])
        rows = [
            tiles[0],
            pltpu.roll(row_1, 32, 1),
            pltpu.roll(row_2, 64, 1),
            pltpu.roll(tiles[2], 96, 1),
        ]
        for offset, row in enumerate(rows):
            start = (4 * quad + offset) * 8
            matrices[start : start + count, :] = jnp.where(lane < NB, row, 0.0)


def prepare_kernel(pairs, table, fock, coupling, fixed, starts, columns, masked, fock_rows, cross_rows):
    unflatten(fock, fock_rows)
    unflatten(coupling, cross_rows)
    base = (pairs[0, 0] // FRAG_DEV) * FRAG_DEV
    lane = iota((NA, 128), 1)
    atom = iota((NA, 128), 0).astype(F32)

    source = iota((N_FRAG, 128), 0) * FRAG_DEV + iota((N_FRAG, 128), 1) // NA
    charges = table[:, 0, :]
    for dimer in range(DIM_DEV):
        hidden = jnp.logical_or(source == pairs[dimer, 0], source == pairs[dimer, 1])
        masked[dimer] = jnp.where(hidden, 0.0, charges)
        for side in range(2):
            fragment = pairs[dimer, side]
            columns[2 * dimer + side] = table[fragment // FRAG_DEV].T

    small_eye = iota((NB, 128), 0) == iota((NB, 128), 1)
    for dimer in range(DIM_DEV):
        own, places = [], []
        for side in range(2):
            local = pl.multiple_of((pairs[dimer, side] % FRAG_DEV) * NA, NA)
            mine = columns[2 * dimer + side, pl.ds(local, NA), :]
            own.append(mine)
            places.append([jnp.broadcast_to(mine[:, k : k + 1], (NA, 128)) for k in (1, 2, 3)])

        def gather(step, sums, dimer=dimer, places=places):
            sums = list(sums)
            for inner in range(BATCH):
                block = step * BATCH + inner
                weight = masked[dimer, pl.ds(block, 1), :]
                spot = [table[block, k : k + 1, :] for k in (1, 2, 3)]
                for side in range(2):
                    delta = [place - here for place, here in zip(places[side], spot)]
                    distance = delta[0] * delta[0] + delta[1] * delta[1] + delta[2] * delta[2]
                    sums[side] += weight * lax.rsqrt(distance + 1.0)
            return tuple(sums)

        zero = jnp.zeros((NA, 128), F32)
        sums = lax.fori_loop(0, N_FRAG // BATCH, gather, (zero, zero))
        start = jnp.zeros((1, 1), F32)
        for side in range(2):
            potential = jnp.sum(sums[side], axis=1, keepdims=True)
            count, population, trace = (own[side][:, k : k + 1] for k in (4, 5, 6))
            scaled = lane.astype(F32) * count
            inside = jnp.logical_and(atom * NB <= scaled, scaled < (atom + 1.0) * NB)
            inside = jnp.logical_and(inside, lane < NB)
            shift = jnp.sum(jnp.where(inside, potential, 0.0), axis=0, keepdims=True)
            shift = jnp.where(small_eye, shift, 0.0)
            if side == 0:
                held = pairs[dimer, 0] - base
                shift += fock_rows[pl.ds(held, NB, stride=8), :]
            fixed[dimer, side * NB : (side + 1) * NB, side * 128 : (side + 1) * 128] = shift
            start += jnp.sum(potential * population + trace, axis=0, keepdims=True)
        starts[dimer : dimer + 1, :] = jnp.broadcast_to(start, (1, 128))
        cross = cross_rows[pl.ds(dimer, NB, stride=8), :]
        fixed[dimer, :NB, 128:256] = cross
        fixed[dimer, NB:, :128] = jnp.concatenate(
            [cross.T[:NB, :], jnp.zeros((NB, 128 - NB), F32)], axis=1
        )


def prepare_dimers(pairs, table, fock, coupling):
    return pl.pallas_call(
        prepare_kernel,
        out_shape=(
            jax.ShapeDtypeStruct((DIM_DEV, 2 * NB, 256), F32),
            jax.ShapeDtypeStruct((8, 128), F32),
        ),
        in_specs=[pl.BlockSpec(memory_space=SMEM)] + [pl.BlockSpec(memory_space=VMEM)] * 3,
        out_specs=(pl.BlockSpec(memory_space=VMEM),) * 2,
        scratch_shapes=[
            VMEM((2 * DIM_DEV, 128, 8), F32),
            VMEM((DIM_DEV, N_FRAG, 128), F32),
            VMEM((8 * NB, 128), F32),
            VMEM((8 * NB, 128), F32),
        ],
        compiler_params=pltpu.CompilerParams(vmem_limit_bytes=8 << 20),
        name="prepare_dimers",
    )(pairs, table, fock, coupling)


def solve_kernel(
    pairs, fixed, starts, fock_0, fock_1, fock_2, fock_3, sent, energies,
    fock_rows, shifted, state, high, low, square_high, square_low,
):
    for far, fock in enumerate((fock_0, fock_1, fock_2, fock_3)):
        fock_rows[far] = fock[...].astype(F32)
    base = (pairs[0, 0] // FRAG_DEV) * FRAG_DEV
    pair_base = (base // NA) * NA
    for buffer in (high, low, square_high, square_low):
        for dimer in range(DIM_DEV):
            buffer[dimer, NB:128, :] = jnp.zeros((128 - NB, 256), BF16)
            buffer[dimer, 128 + NB :, :] = jnp.zeros((128 - NB, 256), BF16)

    rows, cols = iota((2 * NB, 256), 0), iota((2 * NB, 256), 1)
    eye = cols == jnp.where(rows < NB, rows, rows + (128 - NB))
    centres = []
    for dimer in range(DIM_DEV):
        held = pairs[dimer, 1] - base
        part = unpacked(fock_rows[held // FRAG_DEV, pl.ds(held % FRAG_DEV, 48, stride=8), :])
        shifted[dimer, :NB, :] = fixed[dimer, :NB, :]
        shifted[dimer, NB:, :128] = fixed[dimer, NB:, :128]
        shifted[dimer, NB:, 128:] = fixed[dimer, NB:, 128:] + part
        fock = shifted[dimer]
        trace = jnp.sum(jnp.where(eye, fock, 0.0), axis=(0, 1), keepdims=True)
        centre = trace / (2.0 * NB)
        fock = jnp.where(eye, fock - centre, fock)
        width = jnp.max(jnp.sum(jnp.abs(fock), axis=1, keepdims=True), axis=0, keepdims=True) + 1e-06
        shifted[dimer] = fock
        start = fock / width
        state[dimer] = start
        keep(high, low, dimer, start)
        centres.append(centre)

    def purify(step, carry):
        for dimer in range(DIM_DEV):
            square = product(high, low, dimer, high, low)
            keep(square_high, square_low, dimer, square)
        for dimer in range(DIM_DEV):
            cube = product(high, low, dimer, square_high, square_low)
            later = 1.5 * state[dimer] - 0.5 * cube
            state[dimer] = later
            keep(high, low, dimer, later)
        return carry

    lax.fori_loop(0, PURIF, purify, 0, unroll=UNROLL)

    lane_16 = iota((16, 128), 1)
    for dimer in range(DIM_DEV):
        final = state[dimer]
        overlap = jnp.sum(final * shifted[dimer], axis=(0, 1), keepdims=True)
        trace = jnp.sum(jnp.where(eye, final, 0.0), axis=(0, 1), keepdims=True)
        centre = centres[dimer]
        energy = 0.5 * (2.0 * NB * centre - overlap - centre * trace) - starts[dimer : dimer + 1, 0:1]
        energies[dimer : dimer + 1, :] = jnp.broadcast_to(energy, (1, 128))
        for side in range(2):
            slot = side * DIM_DEV + dimer
            block = final[side * NB : (side + 1) * NB, side * 128 : (side + 1) * 128]
            target = (pairs[dimer, side] - pair_base).astype(F32)
            corner = pltpu.roll(block[64:96, :], 32, 1)
            pieces = [
                jnp.where(lane_16 < NB, block[:16, :], corner[:16, :]),
                jnp.where(lane_16 < NB, block[16:32, :], corner[16:, :]),
            ]
            left, right = pltpu.roll(block[32:48, :], 96, 1), pltpu.roll(block[48:64, :], 32, 1)
            piece = jnp.where(lane_16 < 64, left, right)
            piece = jnp.where(lane_16 == ID_LANE, target, piece)
            piece = jnp.where(lane_16 == ONE_LANE, 1.0, piece)
            beside = energy if side == 0 else jnp.zeros((1, 1), F32)
            pieces.append(jnp.where(lane_16 == ENERGY_LANE, beside, piece))
            for part, piece in enumerate(pieces):
                sent[pl.ds(part * 8 + slot, 16, stride=8 * PARTS), :] = piece


def keep(high, low, dimer, value):
    upper, lower = halves(value)
    for buffer, part in ((high, upper), (low, lower)):
        buffer[dimer, :NB, :] = part[:NB]
        buffer[dimer, 128 : 128 + NB, :] = part[NB:]


def product(high, low, dimer, right_high, right_low):
    upper = [high[dimer, :NB, :], high[dimer, 128 : 128 + NB, :]]
    lower = [low[dimer, :NB, :], low[dimer, 128 : 128 + NB, :]]
    both = dot32(jnp.concatenate(upper + lower, axis=0), right_high[dimer])
    cross = dot32(jnp.concatenate(upper, axis=0), right_low[dimer])
    return both[: 2 * NB] + (both[2 * NB :] + cross)


def solve_dimers(pairs, fixed, starts, focks):
    matrix = (DIM_DEV, 2 * NB, 256)
    split = (DIM_DEV, 256, 256)
    return pl.pallas_call(
        solve_kernel,
        out_shape=(
            jax.ShapeDtypeStruct((N_TEAM * 8 * PARTS, 128), F32),
            jax.ShapeDtypeStruct((8, 128), F32),
        ),
        in_specs=[pl.BlockSpec(memory_space=SMEM)] + [pl.BlockSpec(memory_space=VMEM)] * 6,
        out_specs=(pl.BlockSpec(memory_space=VMEM),) * 2,
        scratch_shapes=[
            VMEM((REACH + 1, 48 * FRAG_DEV, 128), F32),
            VMEM(matrix, F32),
            VMEM(matrix, F32),
            VMEM(split, BF16),
            VMEM(split, BF16),
            VMEM(split, BF16),
            VMEM(split, BF16),
        ],
        compiler_params=pltpu.CompilerParams(vmem_limit_bytes=20 << 20),
        name="solve_dimers",
    )(pairs, fixed, starts, *focks)


def sort_kernel(arrived, own, next_1, next_2, energy):
    parts = [
        arrived[:, part * 8 : (part + 1) * 8, :].reshape(N_TEAM * 8, 128) for part in range(PARTS)
    ]
    target = parts[2][:, ID_LANE : ID_LANE + 1].astype(jnp.int32)
    chosen = jnp.where(iota((128, 64), 1) == target, 1.0, 0.0).astype(BF16)
    value = jnp.concatenate(parts, axis=1)
    upper = value.astype(BF16)
    rest = value - upper.astype(F32)
    middle = rest.astype(BF16)
    lower = (rest - middle.astype(F32)).astype(BF16)
    total = jnp.zeros((64, 128 * PARTS), F32)
    for piece in (lower, middle, upper):
        total += lax.dot_general(
            chosen, piece, (((0,), (0,)), ((), ())), preferred_element_type=F32
        )
    own[...] = total[:16]
    next_1[...] = total[16:32].astype(BF16)
    next_2[...] = total[32:48].astype(BF16)
    summed = jnp.sum(parts[2], axis=0, keepdims=True)
    energy[...] = jnp.broadcast_to(summed, (8, 128))


def sort_blocks(arrived):
    return pl.pallas_call(
        sort_kernel,
        out_shape=(
            jax.ShapeDtypeStruct((16, 128 * PARTS), F32),
            jax.ShapeDtypeStruct((16, 128 * PARTS), BF16),
            jax.ShapeDtypeStruct((16, 128 * PARTS), BF16),
            jax.ShapeDtypeStruct((8, 128), F32),
        ),
        in_specs=[pl.BlockSpec(memory_space=VMEM)],
        out_specs=(pl.BlockSpec(memory_space=VMEM),) * 4,
        compiler_params=pltpu.CompilerParams(vmem_limit_bytes=4 << 20),
        name="sort_blocks",
    )(arrived)


def join_kernel(own, from_1, from_2, energy, sent):
    total = own[...] + from_1[...].astype(F32) + from_2[...].astype(F32)
    lane = iota((8, 128), 1)
    mine = jnp.broadcast_to(energy[0:1, ENERGY_LANE : ENERGY_LANE + 1], (8, 128))
    for core in range(2):
        for part in range(PARTS):
            rows = total[core * 8 : core * 8 + 8, part * 128 : (part + 1) * 128]
            if part == 2:
                rows = jnp.where(lane == SUM_LANE, mine, rows)
            for group in range(N_GRP):
                sent[2 * group + core, part * 8 : (part + 1) * 8, :] = rows


def join_blocks(own, from_1, from_2, energy):
    return pl.pallas_call(
        join_kernel,
        out_shape=jax.ShapeDtypeStruct((N_TEAM, 8 * PARTS, 128), F32),
        in_specs=[pl.BlockSpec(memory_space=VMEM)] * 4,
        out_specs=pl.BlockSpec(memory_space=VMEM),
        compiler_params=pltpu.CompilerParams(vmem_limit_bytes=4 << 20),
        name="join_blocks",
    )(own, from_1, from_2, energy)


def unpack_kernel(arrived, dens, energy_rows, out, total, energies, turned):
    for dimer in range(DIM_DEV):
        energies[dimer] = jnp.sum(energy_rows[dimer : dimer + 1, 0:1])
    for fragment in range(FRAG_DEV):
        rows = [
            arrived[pl.ds(part * 8 + fragment, 16, stride=8 * PARTS), :] for part in range(PARTS)
        ]
        turned[pl.ds(fragment, NB, stride=8), :] = unpacked(jnp.concatenate(rows, axis=0))
    lane = iota((8, 128), 1)
    number = arrived[16:24, ONE_LANE : ONE_LANE + 1]
    number = jnp.broadcast_to(number, (8, 128))
    half_number = 0.5 * number

    def matrix_row(row):
        return turned[row * 8 : row * 8 + 8, :]

    def finish(tile, value):
        here = slice(tile * 128, (tile + 1) * 128)
        first = (-tile * 128) % (NB + 1)
        on_diagonal = jnp.logical_or(lane == first, lane == first + NB + 1)
        value = -0.5 * value - number * dens[:, here].astype(F32)
        out[:, here] = value + jnp.where(on_diagonal, half_number, 0.0)

    for quad in range(NB // 4):
        row_0 = matrix_row(4 * quad)
        row_1 = pltpu.roll(matrix_row(4 * quad + 1), 96, 1)
        row_2 = pltpu.roll(matrix_row(4 * quad + 2), 64, 1)
        row_3 = pltpu.roll(matrix_row(4 * quad + 3), 32, 1)
        finish(3 * quad, jnp.where(lane < 96, row_0, row_1))
        finish(3 * quad + 1, jnp.where(lane < 64, row_1, row_2))
        finish(3 * quad + 2, jnp.where(lane < 32, row_2, row_3))

    energy = jnp.zeros((1, 128), F32)
    for member in range(N_TEAM):
        start = member * 8 * PARTS + 16
        energy += arrived[start : start + 1, :]
    total[0] = jnp.sum(energy[:, SUM_LANE : SUM_LANE + 1])


def unpack_blocks(arrived, density, energies):
    return pl.pallas_call(
        unpack_kernel,
        out_shape=(
            jax.ShapeDtypeStruct((FRAG_DEV, FLAT), F32),
            jax.ShapeDtypeStruct((1,), F32),
            jax.ShapeDtypeStruct((DIM_DEV,), F32),
        ),
        in_specs=[pl.BlockSpec(memory_space=VMEM)] * 3,
        out_specs=(
            pl.BlockSpec(memory_space=VMEM),
            pl.BlockSpec(memory_space=SMEM),
            pl.BlockSpec(memory_space=SMEM),
        ),
        scratch_shapes=[VMEM((8 * NB, 128), F32)],
        compiler_params=pltpu.CompilerParams(vmem_limit_bytes=4 << 20),
        name="unpack_blocks",
    )(arrived.reshape(N_TEAM * 8 * PARTS, 128), density, energies)


def energy_moves():
    moves = []
    for group in range(N_GRP):
        for pair in range(N_PAIR):
            for core in range(2):
                source = group * N_FRAG + pair * 2 + core
                away = (pair + 2 * group + core) % N_PAIR
                moves.append((source, group * N_FRAG + away * 2 + core))
    return moves


def per_device(density, fock_blocks, coupling, dimer_pairs, atom_counts, nuclear_charge, coords):
    table, packed = atom_table(density, fock_blocks, nuclear_charge, atom_counts, coords)
    focks = [packed]
    for distance in range(1, REACH + 1):
        moves = [(index + distance, index) for index in range(N_FRAG - distance)]
        focks.append(lax.ppermute(packed, FRAG, moves))
    table = exchange(table, FRAG)
    fixed, starts = prepare_dimers(dimer_pairs, table, fock_blocks, coupling)
    sent, energies = solve_dimers(dimer_pairs, fixed, starts, focks)
    arrived = exchange(sent.reshape(N_TEAM, 8 * PARTS, 128), TEAM)
    own, next_1, next_2, energy = sort_blocks(arrived)
    from_1 = lax.ppermute(next_1, PAIR, [(index, index + 1) for index in range(N_PAIR - 1)])
    from_2 = lax.ppermute(next_2, PAIR, [(index, index + 2) for index in range(N_PAIR - 2)])
    energy = lax.ppermute(energy, GRP_FRAG, energy_moves())
    arrived = exchange(join_blocks(own, from_1, from_2, energy), TEAM)
    correction, total, energies = unpack_blocks(arrived, density, energies)
    return correction, energies, total.reshape(())


def solution(mesh):
    finer = Mesh(
        mesh.devices.reshape(2, 4, 2, 8, 2), ("grp_0", "grp_1", "frag_0", "frag_1", "frag_2")
    )
    return jax.shard_map(
        per_device,
        mesh=finer,
        in_specs=(
            P(FRAG, None),
            P(FRAG, None),
            P(GRP_FRAG, None),
            P(GRP_FRAG, None),
            P(FRAG),
            P(FRAG),
            P(None, FRAG),
        ),
        out_specs=(P(FRAG, None), P(GRP_FRAG), P()),
        check_vma=False,
    )
```

```python
import jax
import jax.numpy as jnp
from jax import lax
from jax.experimental import pallas as pl
from jax.experimental.pallas import tpu as pltpu
from jax.sharding import Mesh
from jax.sharding import PartitionSpec as P

NB = 96
NA = 16
REACH = 3
PURIF = 12
UNROLL = 12
BATCH = 16
FRAG_DEV = 8
DIM_DEV = 4
FLAT = NB * NB
FRAG = ("frag_0", "frag_1", "frag_2")
PAIR = ("frag_0", "frag_1")
GRP_FRAG = ("grp_0", "grp_1", "frag_0", "frag_1", "frag_2")
TEAM = ("grp_0", "grp_1", "frag_2")
N_FRAG = 32
N_PAIR = 16
N_TEAM = 16
N_GRP = 8
F32 = jnp.float32
BF16 = jnp.bfloat16
VMEM = pltpu.VMEM
SMEM = pltpu.SMEM

PARTS = 3
ID_LANE = 64
ONE_LANE = 65
ENERGY_LANE = 66
SUM_LANE = 67


def iota(shape, dim):
    return lax.broadcasted_iota(jnp.int32, shape, dim)


def exchange(value, axis):
    return lax.all_to_all(value, axis, split_axis=0, concat_axis=0, tiled=True)


def dot32(left, right):
    return jnp.dot(left, right, preferred_element_type=F32)


def halves(value):
    high = value.astype(BF16)
    return high, (value - high.astype(F32)).astype(BF16)


def table_kernel(counts, dens, fock, nuclear, coords, table, packed, matrices):
    lane = iota((1, 128), 1)
    trace_sum = jnp.zeros((FRAG_DEV, 128), F32)
    diagonal = jnp.zeros((FRAG_DEV, 128), F32)
    for chunk in range(FLAT // 128):
        here = slice(chunk * 128, (chunk + 1) * 128)
        block = dens[:, here].astype(F32)
        trace_sum += block * fock[:, here].astype(F32)
        first = (-chunk * 128) % (NB + 1)
        on_diagonal = jnp.logical_or(lane == first, lane == first + NB + 1)
        diagonal += jnp.where(on_diagonal, block, 0.0)
    fragment = lane // NA
    atom = (lane % NA).astype(F32)
    count = jnp.zeros((1, 128), F32)
    for index in range(FRAG_DEV):
        count = jnp.where(fragment == index, counts[index].astype(F32), count)
    basis = (iota((128, 128), 0) * 33) % 128
    scaled = basis.astype(F32) * count
    inside = jnp.logical_and(atom * NB <= scaled, scaled < (atom + 1.0) * NB)
    owner = jnp.where(jnp.logical_and(inside, basis < NB), 1.0, 0.0).astype(BF16)
    spread = dot32(diagonal.astype(BF16), owner)
    own_lane = iota((FRAG_DEV, 128), 0) == fragment
    population = jnp.sum(jnp.where(own_lane, spread, 0.0), axis=0, keepdims=True)
    traces = jnp.sum(trace_sum, axis=1, keepdims=True)
    at_first = jnp.logical_and(own_lane, lane % NA == 0)
    trace_row = jnp.sum(jnp.where(at_first, traces, 0.0), axis=0, keepdims=True)
    live = jnp.where(atom < count, 1.0, 0.0)
    charge = live * nuclear[...] - 2.0 * population
    row = iota((8, 128), 0)
    rows = [charge, coords[0:1, :], coords[1:2, :], coords[2:3, :], count, population, trace_row]
    value = jnp.zeros((8, 128), F32)
    for index, content in enumerate(rows):
        value = jnp.where(row == index, content, value)
    for peer in range(N_FRAG):
        table[peer] = value
    unflatten(fock, matrices)
    pack_rows(matrices, packed)


def pack_rows(matrices, packed):
    lane = iota((8, 128), 1)

    def row(index):
        return matrices[8 * index : 8 * index + 8, :]

    rows = [
        jnp.where(lane < NB, row(index), pltpu.roll(row(64 + index), 32, 1)) for index in range(32)
    ]
    for index in range(16):
        left, right = pltpu.roll(row(32 + index), 96, 1), pltpu.roll(row(48 + index), 32, 1)
        rows.append(jnp.where(lane < 64, left, right))
    for index in range(0, 48, 2):
        both = jnp.concatenate(rows[index : index + 2], axis=0)
        packed[8 * index : 8 * index + 16, :] = both.astype(BF16)


def unpacked(rows):
    lane = iota((32, 128), 1)
    top, middle = rows[:32, :], rows[32:, :]
    turned = jnp.concatenate([rows, jnp.zeros((80, 128), F32)], axis=0).T
    first = jnp.where(lane < NB, top, 0.0)
    beside = jnp.concatenate([pltpu.roll(middle, 32, 1), pltpu.roll(middle, 96, 1)], axis=0)
    second = jnp.where(lane < 32, turned[32:64, :], jnp.where(lane < NB, beside, 0.0))
    mirrored = jnp.logical_and(iota((32, 128), 0) >= 16, jnp.logical_and(lane >= 32, lane < 48))
    second = jnp.where(mirrored, turned[:32, :], second)
    third = jnp.where(lane < NB, pltpu.roll(top, 96, 1), 0.0)
    third = jnp.where(lane < 64, pltpu.roll(turned[96:128, :], 16, 1), third)
    third = jnp.where(lane < 48, turned[32:64, :], third)
    third = jnp.where(lane < 32, turned[64:96, :], third)
    return jnp.concatenate([first, second, third], axis=0)


def atom_table(density, fock_blocks, nuclear_charge, atom_counts, coords):
    return pl.pallas_call(
        table_kernel,
        out_shape=(
            jax.ShapeDtypeStruct((N_FRAG, 8, 128), F32),
            jax.ShapeDtypeStruct((48 * FRAG_DEV, 128), BF16),
        ),
        in_specs=[pl.BlockSpec(memory_space=SMEM)] + [pl.BlockSpec(memory_space=VMEM)] * 4,
        out_specs=(pl.BlockSpec(memory_space=VMEM),) * 2,
        scratch_shapes=[VMEM((8 * NB, 128), F32)],
        name="atom_table",
    )(atom_counts, density, fock_blocks, nuclear_charge.reshape(1, 128), coords)


def unflatten(flat, matrices):
    count = flat.shape[0]
    lane = iota((count, 128), 1)
    for quad in range(NB // 4):
        tiles = []
        for tile in range(3 * quad, 3 * quad + 3):
            tiles.append(flat[:, tile * 128 : (tile + 1) * 128].astype(F32))
        row_1 = jnp.where(lane < 96, tiles[1], tiles[0])
        row_2 = jnp.where(lane < 64, tiles[2], tiles[1])
        rows = [
            tiles[0],
            pltpu.roll(row_1, 32, 1),
            pltpu.roll(row_2, 64, 1),
            pltpu.roll(tiles[2], 96, 1),
        ]
        for offset, row in enumerate(rows):
            start = (4 * quad + offset) * 8
            matrices[start : start + count, :] = jnp.where(lane < NB, row, 0.0)


def prepare_kernel(pairs, table, fock, coupling, fixed, starts, columns, masked, fock_rows, cross_rows):
    unflatten(fock, fock_rows)
    unflatten(coupling, cross_rows)
    base = (pairs[0, 0] // FRAG_DEV) * FRAG_DEV
    lane = iota((NA, 128), 1)
    atom = iota((NA, 128), 0).astype(F32)

    source = iota((N_FRAG, 128), 0) * FRAG_DEV + iota((N_FRAG, 128), 1) // NA
    charges = table[:, 0, :]
    for dimer in range(DIM_DEV):
        hidden = jnp.logical_or(source == pairs[dimer, 0], source == pairs[dimer, 1])
        masked[dimer] = jnp.where(hidden, 0.0, charges)
        for side in range(2):
            fragment = pairs[dimer, side]
            columns[2 * dimer + side] = table[fragment // FRAG_DEV].T

    small_eye = iota((NB, 128), 0) == iota((NB, 128), 1)
    for dimer in range(DIM_DEV):
        own, places = [], []
        for side in range(2):
            local = pl.multiple_of((pairs[dimer, side] % FRAG_DEV) * NA, NA)
            mine = columns[2 * dimer + side, pl.ds(local, NA), :]
            own.append(mine)
            places.append([jnp.broadcast_to(mine[:, k : k + 1], (NA, 128)) for k in (1, 2, 3)])

        def gather(step, sums, dimer=dimer, places=places):
            sums = list(sums)
            for inner in range(BATCH):
                block = step * BATCH + inner
                weight = masked[dimer, pl.ds(block, 1), :]
                spot = [table[block, k : k + 1, :] for k in (1, 2, 3)]
                for side in range(2):
                    delta = [place - here for place, here in zip(places[side], spot)]
                    distance = delta[0] * delta[0] + delta[1] * delta[1] + delta[2] * delta[2]
                    sums[side] += weight * lax.rsqrt(distance + 1.0)
            return tuple(sums)

        zero = jnp.zeros((NA, 128), F32)
        sums = lax.fori_loop(0, N_FRAG // BATCH, gather, (zero, zero))
        start = jnp.zeros((1, 1), F32)
        for side in range(2):
            potential = jnp.sum(sums[side], axis=1, keepdims=True)
            count, population, trace = (own[side][:, k : k + 1] for k in (4, 5, 6))
            scaled = lane.astype(F32) * count
            inside = jnp.logical_and(atom * NB <= scaled, scaled < (atom + 1.0) * NB)
            inside = jnp.logical_and(inside, lane < NB)
            shift = jnp.sum(jnp.where(inside, potential, 0.0), axis=0, keepdims=True)
            shift = jnp.where(small_eye, shift, 0.0)
            if side == 0:
                held = pairs[dimer, 0] - base
                shift += fock_rows[pl.ds(held, NB, stride=8), :]
            fixed[dimer, side * NB : (side + 1) * NB, side * 128 : (side + 1) * 128] = shift
            start += jnp.sum(potential * population + trace, axis=0, keepdims=True)
        starts[dimer : dimer + 1, :] = jnp.broadcast_to(start, (1, 128))
        cross = cross_rows[pl.ds(dimer, NB, stride=8), :]
        fixed[dimer, :NB, 128:256] = cross
        fixed[dimer, NB:, :128] = jnp.concatenate(
            [cross.T[:NB, :], jnp.zeros((NB, 128 - NB), F32)], axis=1
        )


def prepare_dimers(pairs, table, fock, coupling):
    return pl.pallas_call(
        prepare_kernel,
        out_shape=(
            jax.ShapeDtypeStruct((DIM_DEV, 2 * NB, 256), F32),
            jax.ShapeDtypeStruct((8, 128), F32),
        ),
        in_specs=[pl.BlockSpec(memory_space=SMEM)] + [pl.BlockSpec(memory_space=VMEM)] * 3,
        out_specs=(pl.BlockSpec(memory_space=VMEM),) * 2,
        scratch_shapes=[
            VMEM((2 * DIM_DEV, 128, 8), F32),
            VMEM((DIM_DEV, N_FRAG, 128), F32),
            VMEM((8 * NB, 128), F32),
            VMEM((8 * NB, 128), F32),
        ],
        compiler_params=pltpu.CompilerParams(vmem_limit_bytes=8 << 20),
        name="prepare_dimers",
    )(pairs, table, fock, coupling)


def solve_kernel(
    pairs, fixed, starts, fock_0, fock_1, fock_2, fock_3, sent, energies,
    fock_rows, shifted, state, high, low, square_high, square_low,
):
    for far, fock in enumerate((fock_0, fock_1, fock_2, fock_3)):
        fock_rows[far] = fock[...].astype(F32)
    base = (pairs[0, 0] // FRAG_DEV) * FRAG_DEV
    pair_base = (base // NA) * NA
    for buffer in (high, low, square_high, square_low):
        for dimer in range(DIM_DEV):
            buffer[dimer, NB:128, :] = jnp.zeros((128 - NB, 256), BF16)
            buffer[dimer, 128 + NB :, :] = jnp.zeros((128 - NB, 256), BF16)

    rows, cols = iota((2 * NB, 256), 0), iota((2 * NB, 256), 1)
    eye = cols == jnp.where(rows < NB, rows, rows + (128 - NB))
    centres = []
    for dimer in range(DIM_DEV):
        held = pairs[dimer, 1] - base
        part = unpacked(fock_rows[held // FRAG_DEV, pl.ds(held % FRAG_DEV, 48, stride=8), :])
        shifted[dimer, :NB, :] = fixed[dimer, :NB, :]
        shifted[dimer, NB:, :128] = fixed[dimer, NB:, :128]
        shifted[dimer, NB:, 128:] = fixed[dimer, NB:, 128:] + part
        fock = shifted[dimer]
        trace = jnp.sum(jnp.where(eye, fock, 0.0), axis=(0, 1), keepdims=True)
        centre = trace / (2.0 * NB)
        fock = jnp.where(eye, fock - centre, fock)
        width = jnp.max(jnp.sum(jnp.abs(fock), axis=1, keepdims=True), axis=0, keepdims=True) + 1e-06
        shifted[dimer] = fock
        start = fock / width
        state[dimer] = start
        keep(high, low, dimer, start)
        centres.append(centre)

    def purify(step, carry):
        for dimer in range(DIM_DEV):
            square = product(high, low, dimer, high, low)
            keep(square_high, square_low, dimer, square)
        for dimer in range(DIM_DEV):
            cube = product(high, low, dimer, square_high, square_low)
            later = 1.5 * state[dimer] - 0.5 * cube
            state[dimer] = later
            keep(high, low, dimer, later)
        return carry

    lax.fori_loop(0, PURIF, purify, 0, unroll=UNROLL)

    lane_16 = iota((16, 128), 1)
    for dimer in range(DIM_DEV):
        final = state[dimer]
        overlap = jnp.sum(final * shifted[dimer], axis=(0, 1), keepdims=True)
        trace = jnp.sum(jnp.where(eye, final, 0.0), axis=(0, 1), keepdims=True)
        centre = centres[dimer]
        energy = 0.5 * (2.0 * NB * centre - overlap - centre * trace) - starts[dimer : dimer + 1, 0:1]
        energies[dimer : dimer + 1, :] = jnp.broadcast_to(energy, (1, 128))
        for side in range(2):
            slot = side * DIM_DEV + dimer
            block = final[side * NB : (side + 1) * NB, side * 128 : (side + 1) * 128]
            target = (pairs[dimer, side] - pair_base).astype(F32)
            corner = pltpu.roll(block[64:96, :], 32, 1)
            pieces = [
                jnp.where(lane_16 < NB, block[:16, :], corner[:16, :]),
                jnp.where(lane_16 < NB, block[16:32, :], corner[16:, :]),
            ]
            left, right = pltpu.roll(block[32:48, :], 96, 1), pltpu.roll(block[48:64, :], 32, 1)
            piece = jnp.where(lane_16 < 64, left, right)
            piece = jnp.where(lane_16 == ID_LANE, target, piece)
            piece = jnp.where(lane_16 == ONE_LANE, 1.0, piece)
            beside = energy if side == 0 else jnp.zeros((1, 1), F32)
            pieces.append(jnp.where(lane_16 == ENERGY_LANE, beside, piece))
            for part, piece in enumerate(pieces):
                sent[pl.ds(part * 8 + slot, 16, stride=8 * PARTS), :] = piece


def keep(high, low, dimer, value):
    upper, lower = halves(value)
    for buffer, part in ((high, upper), (low, lower)):
        buffer[dimer, :NB, :] = part[:NB]
        buffer[dimer, 128 : 128 + NB, :] = part[NB:]


def product(high, low, dimer, right_high, right_low):
    upper = [high[dimer, :NB, :], high[dimer, 128 : 128 + NB, :]]
    lower = [low[dimer, :NB, :], low[dimer, 128 : 128 + NB, :]]
    both = dot32(jnp.concatenate(upper + lower, axis=0), right_high[dimer])
    cross = dot32(jnp.concatenate(upper, axis=0), right_low[dimer])
    return both[: 2 * NB] + (both[2 * NB :] + cross)


def solve_dimers(pairs, fixed, starts, focks):
    matrix = (DIM_DEV, 2 * NB, 256)
    split = (DIM_DEV, 256, 256)
    return pl.pallas_call(
        solve_kernel,
        out_shape=(
            jax.ShapeDtypeStruct((N_TEAM * 8 * PARTS, 128), F32),
            jax.ShapeDtypeStruct((8, 128), F32),
        ),
        in_specs=[pl.BlockSpec(memory_space=SMEM)] + [pl.BlockSpec(memory_space=VMEM)] * 6,
        out_specs=(pl.BlockSpec(memory_space=VMEM),) * 2,
        scratch_shapes=[
            VMEM((REACH + 1, 48 * FRAG_DEV, 128), F32),
            VMEM(matrix, F32),
            VMEM(matrix, F32),
            VMEM(split, BF16),
            VMEM(split, BF16),
            VMEM(split, BF16),
            VMEM(split, BF16),
        ],
        compiler_params=pltpu.CompilerParams(vmem_limit_bytes=20 << 20),
        name="solve_dimers",
    )(pairs, fixed, starts, *focks)


def sort_kernel(arrived, own, next_1, next_2, energy):
    parts = [
        arrived[:, part * 8 : (part + 1) * 8, :].reshape(N_TEAM * 8, 128) for part in range(PARTS)
    ]
    target = parts[2][:, ID_LANE : ID_LANE + 1].astype(jnp.int32)
    chosen = jnp.where(iota((128, 64), 1) == target, 1.0, 0.0).astype(BF16)
    value = jnp.concatenate(parts, axis=1)
    upper = value.astype(BF16)
    rest = value - upper.astype(F32)
    middle = rest.astype(BF16)
    lower = (rest - middle.astype(F32)).astype(BF16)
    total = jnp.zeros((64, 128 * PARTS), F32)
    for piece in (lower, middle, upper):
        total += lax.dot_general(
            chosen, piece, (((0,), (0,)), ((), ())), preferred_element_type=F32
        )
    own[...] = total[:16]
    next_1[...] = total[16:32].astype(BF16)
    next_2[...] = total[32:48].astype(BF16)
    summed = jnp.sum(parts[2], axis=0, keepdims=True)
    energy[...] = jnp.broadcast_to(summed, (8, 128))


def sort_blocks(arrived):
    return pl.pallas_call(
        sort_kernel,
        out_shape=(
            jax.ShapeDtypeStruct((16, 128 * PARTS), F32),
            jax.ShapeDtypeStruct((16, 128 * PARTS), BF16),
            jax.ShapeDtypeStruct((16, 128 * PARTS), BF16),
            jax.ShapeDtypeStruct((8, 128), F32),
        ),
        in_specs=[pl.BlockSpec(memory_space=VMEM)],
        out_specs=(pl.BlockSpec(memory_space=VMEM),) * 4,
        compiler_params=pltpu.CompilerParams(vmem_limit_bytes=4 << 20),
        name="sort_blocks",
    )(arrived)


def join_kernel(own, from_1, from_2, energy, sent):
    total = own[...] + from_1[...].astype(F32) + from_2[...].astype(F32)
    lane = iota((8, 128), 1)
    mine = jnp.broadcast_to(energy[0:1, ENERGY_LANE : ENERGY_LANE + 1], (8, 128))
    for core in range(2):
        for part in range(PARTS):
            rows = total[core * 8 : core * 8 + 8, part * 128 : (part + 1) * 128]
            if part == 2:
                rows = jnp.where(lane == SUM_LANE, mine, rows)
            for group in range(N_GRP):
                sent[2 * group + core, part * 8 : (part + 1) * 8, :] = rows


def join_blocks(own, from_1, from_2, energy):
    return pl.pallas_call(
        join_kernel,
        out_shape=jax.ShapeDtypeStruct((N_TEAM, 8 * PARTS, 128), F32),
        in_specs=[pl.BlockSpec(memory_space=VMEM)] * 4,
        out_specs=pl.BlockSpec(memory_space=VMEM),
        compiler_params=pltpu.CompilerParams(vmem_limit_bytes=4 << 20),
        name="join_blocks",
    )(own, from_1, from_2, energy)


def unpack_kernel(arrived, dens, energy_rows, out, total, energies, turned):
    for dimer in range(DIM_DEV):
        energies[dimer] = jnp.sum(energy_rows[dimer : dimer + 1, 0:1])
    for fragment in range(FRAG_DEV):
        rows = [
            arrived[pl.ds(part * 8 + fragment, 16, stride=8 * PARTS), :] for part in range(PARTS)
        ]
        turned[pl.ds(fragment, NB, stride=8), :] = unpacked(jnp.concatenate(rows, axis=0))
    lane = iota((8, 128), 1)
    number = arrived[16:24, ONE_LANE : ONE_LANE + 1]
    number = jnp.broadcast_to(number, (8, 128))
    half_number = 0.5 * number

    def matrix_row(row):
        return turned[row * 8 : row * 8 + 8, :]

    def finish(tile, value):
        here = slice(tile * 128, (tile + 1) * 128)
        first = (-tile * 128) % (NB + 1)
        on_diagonal = jnp.logical_or(lane == first, lane == first + NB + 1)
        value = -0.5 * value - number * dens[:, here].astype(F32)
        out[:, here] = value + jnp.where(on_diagonal, half_number, 0.0)

    for quad in range(NB // 4):
        row_0 = matrix_row(4 * quad)
        row_1 = pltpu.roll(matrix_row(4 * quad + 1), 96, 1)
        row_2 = pltpu.roll(matrix_row(4 * quad + 2), 64, 1)
        row_3 = pltpu.roll(matrix_row(4 * quad + 3), 32, 1)
        finish(3 * quad, jnp.where(lane < 96, row_0, row_1))
        finish(3 * quad + 1, jnp.where(lane < 64, row_1, row_2))
        finish(3 * quad + 2, jnp.where(lane < 32, row_2, row_3))

    energy = jnp.zeros((1, 128), F32)
    for member in range(N_TEAM):
        start = member * 8 * PARTS + 16
        energy += arrived[start : start + 1, :]
    total[0] = jnp.sum(energy[:, SUM_LANE : SUM_LANE + 1])


def unpack_blocks(arrived, density, energies):
    return pl.pallas_call(
        unpack_kernel,
        out_shape=(
            jax.ShapeDtypeStruct((FRAG_DEV, FLAT), F32),
            jax.ShapeDtypeStruct((1,), F32),
            jax.ShapeDtypeStruct((DIM_DEV,), F32),
        ),
        in_specs=[pl.BlockSpec(memory_space=VMEM)] * 3,
        out_specs=(
            pl.BlockSpec(memory_space=VMEM),
            pl.BlockSpec(memory_space=SMEM),
            pl.BlockSpec(memory_space=SMEM),
        ),
        scratch_shapes=[VMEM((8 * NB, 128), F32)],
        compiler_params=pltpu.CompilerParams(vmem_limit_bytes=4 << 20),
        name="unpack_blocks",
    )(arrived.reshape(N_TEAM * 8 * PARTS, 128), density, energies)


def energy_moves():
    moves = []
    for group in range(N_GRP):
        for pair in range(N_PAIR):
            for core in range(2):
                source = group * N_FRAG + pair * 2 + core
                away = (pair + 2 * group + core) % N_PAIR
                moves.append((source, group * N_FRAG + away * 2 + core))
    return moves


def per_device(density, fock_blocks, coupling, dimer_pairs, atom_counts, nuclear_charge, coords):
    table, packed = atom_table(density, fock_blocks, nuclear_charge, atom_counts, coords)
    focks = [packed]
    for distance in range(1, REACH + 1):
        moves = [(index + distance, index) for index in range(N_FRAG - distance)]
        focks.append(lax.ppermute(packed, FRAG, moves))
    table = exchange(table, FRAG)
    fixed, starts = prepare_dimers(dimer_pairs, table, fock_blocks, coupling)
    sent, energies = solve_dimers(dimer_pairs, fixed, starts, focks)
    arrived = exchange(sent.reshape(N_TEAM, 8 * PARTS, 128), TEAM)
    own, next_1, next_2, energy = sort_blocks(arrived)
    from_1 = lax.ppermute(next_1, PAIR, [(index, index + 1) for index in range(N_PAIR - 1)])
    from_2 = lax.ppermute(next_2, PAIR, [(index, index + 2) for index in range(N_PAIR - 2)])
    energy = lax.ppermute(energy, GRP_FRAG, energy_moves())
    arrived = exchange(join_blocks(own, from_1, from_2, energy), TEAM)
    correction, total, energies = unpack_blocks(arrived, density, energies)
    return correction, energies, total.reshape(())


def solution(mesh):
    finer = Mesh(
        mesh.devices.reshape(2, 4, 2, 8, 2), ("grp_0", "grp_1", "frag_0", "frag_1", "frag_2")
    )
    return jax.shard_map(
        per_device,
        mesh=finer,
        in_specs=(
            P(FRAG, None),
            P(FRAG, None),
            P(GRP_FRAG, None),
            P(GRP_FRAG, None),
            P(FRAG),
            P(FRAG),
            P(None, FRAG),
        ),
        out_specs=(P(FRAG, None), P(GRP_FRAG), P()),
        check_vma=False,
    )
```

```python
import jax
import jax.numpy as jnp
from jax import lax
from jax.experimental import pallas as pl
from jax.experimental.pallas import tpu as pltpu
from jax.sharding import Mesh
from jax.sharding import PartitionSpec as P

NB = 96
NA = 16
REACH = 3
PURIF = 12
UNROLL = 12
BATCH = 32
FRAG_DEV = 8
DIM_DEV = 4
FLAT = NB * NB
FRAG = ("frag_0", "frag_1", "frag_2")
PAIR = ("frag_0", "frag_1")
GRP_FRAG = ("grp_0", "grp_1", "frag_0", "frag_1", "frag_2")
TEAM = ("grp_0", "grp_1", "frag_2")
N_FRAG = 32
N_PAIR = 16
N_TEAM = 16
N_GRP = 8
F32 = jnp.float32
BF16 = jnp.bfloat16
VMEM = pltpu.VMEM
SMEM = pltpu.SMEM

PARTS = 3
ID_LANE = 64
ONE_LANE = 65
ENERGY_LANE = 66
SUM_LANE = 67


def iota(shape, dim):
    return lax.broadcasted_iota(jnp.int32, shape, dim)


def exchange(value, axis):
    return lax.all_to_all(value, axis, split_axis=0, concat_axis=0, tiled=True)


def dot32(left, right):
    return jnp.dot(left, right, preferred_element_type=F32)


def halves(value):
    high = value.astype(BF16)
    return high, (value - high.astype(F32)).astype(BF16)


def table_kernel(counts, dens, fock, nuclear, coords, table, packed, matrices):
    lane = iota((1, 128), 1)
    trace_sum = jnp.zeros((FRAG_DEV, 128), F32)
    diagonal = jnp.zeros((FRAG_DEV, 128), F32)
    for chunk in range(FLAT // 128):
        here = slice(chunk * 128, (chunk + 1) * 128)
        block = dens[:, here].astype(F32)
        trace_sum += block * fock[:, here].astype(F32)
        first = (-chunk * 128) % (NB + 1)
        on_diagonal = jnp.logical_or(lane == first, lane == first + NB + 1)
        diagonal += jnp.where(on_diagonal, block, 0.0)
    fragment = lane // NA
    atom = (lane % NA).astype(F32)
    count = jnp.zeros((1, 128), F32)
    for index in range(FRAG_DEV):
        count = jnp.where(fragment == index, counts[index].astype(F32), count)
    basis = (iota((128, 128), 0) * 33) % 128
    scaled = basis.astype(F32) * count
    inside = jnp.logical_and(atom * NB <= scaled, scaled < (atom + 1.0) * NB)
    owner = jnp.where(jnp.logical_and(inside, basis < NB), 1.0, 0.0).astype(BF16)
    spread = dot32(diagonal.astype(BF16), owner)
    own_lane = iota((FRAG_DEV, 128), 0) == fragment
    population = jnp.sum(jnp.where(own_lane, spread, 0.0), axis=0, keepdims=True)
    traces = jnp.sum(trace_sum, axis=1, keepdims=True)
    at_first = jnp.logical_and(own_lane, lane % NA == 0)
    trace_row = jnp.sum(jnp.where(at_first, traces, 0.0), axis=0, keepdims=True)
    live = jnp.where(atom < count, 1.0, 0.0)
    charge = live * nuclear[...] - 2.0 * population
    row = iota((8, 128), 0)
    rows = [charge, coords[0:1, :], coords[1:2, :], coords[2:3, :], count, population, trace_row]
    value = jnp.zeros((8, 128), F32)
    for index, content in enumerate(rows):
        value = jnp.where(row == index, content, value)
    for peer in range(N_FRAG):
        table[peer] = value
    unflatten(fock, matrices)
    pack_rows(matrices, packed)


def pack_rows(matrices, packed):
    lane = iota((8, 128), 1)

    def row(index):
        return matrices[8 * index : 8 * index + 8, :]

    rows = [
        jnp.where(lane < NB, row(index), pltpu.roll(row(64 + index), 32, 1)) for index in range(32)
    ]
    for index in range(16):
        left, right = pltpu.roll(row(32 + index), 96, 1), pltpu.roll(row(48 + index), 32, 1)
        rows.append(jnp.where(lane < 64, left, right))
    for index in range(0, 48, 2):
        both = jnp.concatenate(rows[index : index + 2], axis=0)
        packed[8 * index : 8 * index + 16, :] = both.astype(BF16)


def unpacked(rows):
    lane = iota((32, 128), 1)
    top, middle = rows[:32, :], rows[32:, :]
    turned = jnp.concatenate([rows, jnp.zeros((80, 128), F32)], axis=0).T
    first = jnp.where(lane < NB, top, 0.0)
    beside = jnp.concatenate([pltpu.roll(middle, 32, 1), pltpu.roll(middle, 96, 1)], axis=0)
    second = jnp.where(lane < 32, turned[32:64, :], jnp.where(lane < NB, beside, 0.0))
    mirrored = jnp.logical_and(iota((32, 128), 0) >= 16, jnp.logical_and(lane >= 32, lane < 48))
    second = jnp.where(mirrored, turned[:32, :], second)
    third = jnp.where(lane < NB, pltpu.roll(top, 96, 1), 0.0)
    third = jnp.where(lane < 64, pltpu.roll(turned[96:128, :], 16, 1), third)
    third = jnp.where(lane < 48, turned[32:64, :], third)
    third = jnp.where(lane < 32, turned[64:96, :], third)
    return jnp.concatenate([first, second, third], axis=0)


def atom_table(density, fock_blocks, nuclear_charge, atom_counts, coords):
    return pl.pallas_call(
        table_kernel,
        out_shape=(
            jax.ShapeDtypeStruct((N_FRAG, 8, 128), F32),
            jax.ShapeDtypeStruct((48 * FRAG_DEV, 128), BF16),
        ),
        in_specs=[pl.BlockSpec(memory_space=SMEM)] + [pl.BlockSpec(memory_space=VMEM)] * 4,
        out_specs=(pl.BlockSpec(memory_space=VMEM),) * 2,
        scratch_shapes=[VMEM((8 * NB, 128), F32)],
        name="atom_table",
    )(atom_counts, density, fock_blocks, nuclear_charge.reshape(1, 128), coords)


def unflatten(flat, matrices):
    count = flat.shape[0]
    lane = iota((count, 128), 1)
    for quad in range(NB // 4):
        tiles = []
        for tile in range(3 * quad, 3 * quad + 3):
            tiles.append(flat[:, tile * 128 : (tile + 1) * 128].astype(F32))
        row_1 = jnp.where(lane < 96, tiles[1], tiles[0])
        row_2 = jnp.where(lane < 64, tiles[2], tiles[1])
        rows = [
            tiles[0],
            pltpu.roll(row_1, 32, 1),
            pltpu.roll(row_2, 64, 1),
            pltpu.roll(tiles[2], 96, 1),
        ]
        for offset, row in enumerate(rows):
            start = (4 * quad + offset) * 8
            matrices[start : start + count, :] = jnp.where(lane < NB, row, 0.0)


def prepare_kernel(pairs, table, fock, coupling, fixed, starts, columns, masked, fock_rows, cross_rows):
    unflatten(fock, fock_rows)
    unflatten(coupling, cross_rows)
    base = (pairs[0, 0] // FRAG_DEV) * FRAG_DEV
    lane = iota((NA, 128), 1)
    atom = iota((NA, 128), 0).astype(F32)

    source = iota((N_FRAG, 128), 0) * FRAG_DEV + iota((N_FRAG, 128), 1) // NA
    charges = table[:, 0, :]
    for dimer in range(DIM_DEV):
        hidden = jnp.logical_or(source == pairs[dimer, 0], source == pairs[dimer, 1])
        masked[dimer] = jnp.where(hidden, 0.0, charges)
        for side in range(2):
            fragment = pairs[dimer, side]
            columns[2 * dimer + side] = table[fragment // FRAG_DEV].T

    small_eye = iota((NB, 128), 0) == iota((NB, 128), 1)
    for dimer in range(DIM_DEV):
        own, places = [], []
        for side in range(2):
            local = pl.multiple_of((pairs[dimer, side] % FRAG_DEV) * NA, NA)
            mine = columns[2 * dimer + side, pl.ds(local, NA), :]
            own.append(mine)
            places.append([jnp.broadcast_to(mine[:, k : k + 1], (NA, 128)) for k in (1, 2, 3)])

        def gather(step, sums, dimer=dimer, places=places):
            sums = list(sums)
            for inner in range(BATCH):
                block = step * BATCH + inner
                weight = masked[dimer, pl.ds(block, 1), :]
                spot = [table[block, k : k + 1, :] for k in (1, 2, 3)]
                for side in range(2):
                    delta = [place - here for place, here in zip(places[side], spot)]
                    distance = delta[0] * delta[0] + delta[1] * delta[1] + delta[2] * delta[2]
                    sums[side] += weight * lax.rsqrt(distance + 1.0)
            return tuple(sums)

        zero = jnp.zeros((NA, 128), F32)
        sums = lax.fori_loop(0, N_FRAG // BATCH, gather, (zero, zero))
        start = jnp.zeros((1, 1), F32)
        for side in range(2):
            potential = jnp.sum(sums[side], axis=1, keepdims=True)
            count, population, trace = (own[side][:, k : k + 1] for k in (4, 5, 6))
            scaled = lane.astype(F32) * count
            inside = jnp.logical_and(atom * NB <= scaled, scaled < (atom + 1.0) * NB)
            inside = jnp.logical_and(inside, lane < NB)
            shift = jnp.sum(jnp.where(inside, potential, 0.0), axis=0, keepdims=True)
            shift = jnp.where(small_eye, shift, 0.0)
            if side == 0:
                held = pairs[dimer, 0] - base
                shift += fock_rows[pl.ds(held, NB, stride=8), :]
            fixed[dimer, side * NB : (side + 1) * NB, side * 128 : (side + 1) * 128] = shift
            start += jnp.sum(potential * population + trace, axis=0, keepdims=True)
        starts[dimer : dimer + 1, :] = jnp.broadcast_to(start, (1, 128))
        cross = cross_rows[pl.ds(dimer, NB, stride=8), :]
        fixed[dimer, :NB, 128:256] = cross
        fixed[dimer, NB:, :128] = jnp.concatenate(
            [cross.T[:NB, :], jnp.zeros((NB, 128 - NB), F32)], axis=1
        )


def prepare_dimers(pairs, table, fock, coupling):
    return pl.pallas_call(
        prepare_kernel,
        out_shape=(
            jax.ShapeDtypeStruct((DIM_DEV, 2 * NB, 256), F32),
            jax.ShapeDtypeStruct((8, 128), F32),
        ),
        in_specs=[pl.BlockSpec(memory_space=SMEM)] + [pl.BlockSpec(memory_space=VMEM)] * 3,
        out_specs=(pl.BlockSpec(memory_space=VMEM),) * 2,
        scratch_shapes=[
            VMEM((2 * DIM_DEV, 128, 8), F32),
            VMEM((DIM_DEV, N_FRAG, 128), F32),
            VMEM((8 * NB, 128), F32),
            VMEM((8 * NB, 128), F32),
        ],
        compiler_params=pltpu.CompilerParams(vmem_limit_bytes=8 << 20),
        name="prepare_dimers",
    )(pairs, table, fock, coupling)


def solve_kernel(
    pairs, fixed, starts, fock_0, fock_1, fock_2, fock_3, sent, energies,
    fock_rows, shifted, state, high, low, square_high, square_low,
):
    for far, fock in enumerate((fock_0, fock_1, fock_2, fock_3)):
        fock_rows[far] = fock[...].astype(F32)
    base = (pairs[0, 0] // FRAG_DEV) * FRAG_DEV
    pair_base = (base // NA) * NA
    for buffer in (high, low, square_high, square_low):
        for dimer in range(DIM_DEV):
            buffer[dimer, NB:128, :] = jnp.zeros((128 - NB, 256), BF16)
            buffer[dimer, 128 + NB :, :] = jnp.zeros((128 - NB, 256), BF16)

    rows, cols = iota((2 * NB, 256), 0), iota((2 * NB, 256), 1)
    eye = cols == jnp.where(rows < NB, rows, rows + (128 - NB))
    centres = []
    for dimer in range(DIM_DEV):
        held = pairs[dimer, 1] - base
        part = unpacked(fock_rows[held // FRAG_DEV, pl.ds(held % FRAG_DEV, 48, stride=8), :])
        shifted[dimer, :NB, :] = fixed[dimer, :NB, :]
        shifted[dimer, NB:, :128] = fixed[dimer, NB:, :128]
        shifted[dimer, NB:, 128:] = fixed[dimer, NB:, 128:] + part
        fock = shifted[dimer]
        trace = jnp.sum(jnp.where(eye, fock, 0.0), axis=(0, 1), keepdims=True)
        centre = trace / (2.0 * NB)
        fock = jnp.where(eye, fock - centre, fock)
        width = jnp.max(jnp.sum(jnp.abs(fock), axis=1, keepdims=True), axis=0, keepdims=True) + 1e-06
        shifted[dimer] = fock
        start = fock / width
        state[dimer] = start
        keep(high, low, dimer, start)
        centres.append(centre)

    def purify(step, carry):
        for dimer in range(DIM_DEV):
            square = product(high, low, dimer, high, low)
            keep(square_high, square_low, dimer, square)
        for dimer in range(DIM_DEV):
            cube = product(high, low, dimer, square_high, square_low)
            later = 1.5 * state[dimer] - 0.5 * cube
            state[dimer] = later
            keep(high, low, dimer, later)
        return carry

    lax.fori_loop(0, PURIF, purify, 0, unroll=UNROLL)

    lane_16 = iota((16, 128), 1)
    for dimer in range(DIM_DEV):
        final = state[dimer]
        overlap = jnp.sum(final * shifted[dimer], axis=(0, 1), keepdims=True)
        trace = jnp.sum(jnp.where(eye, final, 0.0), axis=(0, 1), keepdims=True)
        centre = centres[dimer]
        energy = 0.5 * (2.0 * NB * centre - overlap - centre * trace) - starts[dimer : dimer + 1, 0:1]
        energies[dimer : dimer + 1, :] = jnp.broadcast_to(energy, (1, 128))
        for side in range(2):
            slot = side * DIM_DEV + dimer
            block = final[side * NB : (side + 1) * NB, side * 128 : (side + 1) * 128]
            target = (pairs[dimer, side] - pair_base).astype(F32)
            corner = pltpu.roll(block[64:96, :], 32, 1)
            pieces = [
                jnp.where(lane_16 < NB, block[:16, :], corner[:16, :]),
                jnp.where(lane_16 < NB, block[16:32, :], corner[16:, :]),
            ]
            left, right = pltpu.roll(block[32:48, :], 96, 1), pltpu.roll(block[48:64, :], 32, 1)
            piece = jnp.where(lane_16 < 64, left, right)
            piece = jnp.where(lane_16 == ID_LANE, target, piece)
            piece = jnp.where(lane_16 == ONE_LANE, 1.0, piece)
            beside = energy if side == 0 else jnp.zeros((1, 1), F32)
            pieces.append(jnp.where(lane_16 == ENERGY_LANE, beside, piece))
            for part, piece in enumerate(pieces):
                sent[pl.ds(part * 8 + slot, 16, stride=8 * PARTS), :] = piece


def keep(high, low, dimer, value):
    upper, lower = halves(value)
    for buffer, part in ((high, upper), (low, lower)):
        buffer[dimer, :NB, :] = part[:NB]
        buffer[dimer, 128 : 128 + NB, :] = part[NB:]


def product(high, low, dimer, right_high, right_low):
    upper = [high[dimer, :NB, :], high[dimer, 128 : 128 + NB, :]]
    lower = [low[dimer, :NB, :], low[dimer, 128 : 128 + NB, :]]
    both = dot32(jnp.concatenate(upper + lower, axis=0), right_high[dimer])
    cross = dot32(jnp.concatenate(upper, axis=0), right_low[dimer])
    return both[: 2 * NB] + (both[2 * NB :] + cross)


def solve_dimers(pairs, fixed, starts, focks):
    matrix = (DIM_DEV, 2 * NB, 256)
    split = (DIM_DEV, 256, 256)
    return pl.pallas_call(
        solve_kernel,
        out_shape=(
            jax.ShapeDtypeStruct((N_TEAM * 8 * PARTS, 128), F32),
            jax.ShapeDtypeStruct((8, 128), F32),
        ),
        in_specs=[pl.BlockSpec(memory_space=SMEM)] + [pl.BlockSpec(memory_space=VMEM)] * 6,
        out_specs=(pl.BlockSpec(memory_space=VMEM),) * 2,
        scratch_shapes=[
            VMEM((REACH + 1, 48 * FRAG_DEV, 128), F32),
            VMEM(matrix, F32),
            VMEM(matrix, F32),
            VMEM(split, BF16),
            VMEM(split, BF16),
            VMEM(split, BF16),
            VMEM(split, BF16),
        ],
        compiler_params=pltpu.CompilerParams(vmem_limit_bytes=20 << 20),
        name="solve_dimers",
    )(pairs, fixed, starts, *focks)


def sort_kernel(arrived, own, next_1, next_2, energy):
    parts = [
        arrived[:, part * 8 : (part + 1) * 8, :].reshape(N_TEAM * 8, 128) for part in range(PARTS)
    ]
    target = parts[2][:, ID_LANE : ID_LANE + 1].astype(jnp.int32)
    chosen = jnp.where(iota((128, 64), 1) == target, 1.0, 0.0).astype(BF16)
    value = jnp.concatenate(parts, axis=1)
    upper = value.astype(BF16)
    rest = value - upper.astype(F32)
    middle = rest.astype(BF16)
    lower = (rest - middle.astype(F32)).astype(BF16)
    total = jnp.zeros((64, 128 * PARTS), F32)
    for piece in (lower, middle, upper):
        total += lax.dot_general(
            chosen, piece, (((0,), (0,)), ((), ())), preferred_element_type=F32
        )
    own[...] = total[:16]
    next_1[...] = total[16:32].astype(BF16)
    next_2[...] = total[32:48].astype(BF16)
    summed = jnp.sum(parts[2], axis=0, keepdims=True)
    energy[...] = jnp.broadcast_to(summed, (8, 128))


def sort_blocks(arrived):
    return pl.pallas_call(
        sort_kernel,
        out_shape=(
            jax.ShapeDtypeStruct((16, 128 * PARTS), F32),
            jax.ShapeDtypeStruct((16, 128 * PARTS), BF16),
            jax.ShapeDtypeStruct((16, 128 * PARTS), BF16),
            jax.ShapeDtypeStruct((8, 128), F32),
        ),
        in_specs=[pl.BlockSpec(memory_space=VMEM)],
        out_specs=(pl.BlockSpec(memory_space=VMEM),) * 4,
        compiler_params=pltpu.CompilerParams(vmem_limit_bytes=4 << 20),
        name="sort_blocks",
    )(arrived)


def join_kernel(own, from_1, from_2, energy, sent):
    total = own[...] + from_1[...].astype(F32) + from_2[...].astype(F32)
    lane = iota((8, 128), 1)
    mine = jnp.broadcast_to(energy[0:1, ENERGY_LANE : ENERGY_LANE + 1], (8, 128))
    for core in range(2):
        for part in range(PARTS):
            rows = total[core * 8 : core * 8 + 8, part * 128 : (part + 1) * 128]
            if part == 2:
                rows = jnp.where(lane == SUM_LANE, mine, rows)
            for group in range(N_GRP):
                sent[2 * group + core, part * 8 : (part + 1) * 8, :] = rows


def join_blocks(own, from_1, from_2, energy):
    return pl.pallas_call(
        join_kernel,
        out_shape=jax.ShapeDtypeStruct((N_TEAM, 8 * PARTS, 128), F32),
        in_specs=[pl.BlockSpec(memory_space=VMEM)] * 4,
        out_specs=pl.BlockSpec(memory_space=VMEM),
        compiler_params=pltpu.CompilerParams(vmem_limit_bytes=4 << 20),
        name="join_blocks",
    )(own, from_1, from_2, energy)


def unpack_kernel(arrived, dens, energy_rows, out, total, energies, turned):
    for dimer in range(DIM_DEV):
        energies[dimer] = jnp.sum(energy_rows[dimer : dimer + 1, 0:1])
    for fragment in range(FRAG_DEV):
        rows = [
            arrived[pl.ds(part * 8 + fragment, 16, stride=8 * PARTS), :] for part in range(PARTS)
        ]
        turned[pl.ds(fragment, NB, stride=8), :] = unpacked(jnp.concatenate(rows, axis=0))
    lane = iota((8, 128), 1)
    number = arrived[16:24, ONE_LANE : ONE_LANE + 1]
    number = jnp.broadcast_to(number, (8, 128))
    half_number = 0.5 * number

    def matrix_row(row):
        return turned[row * 8 : row * 8 + 8, :]

    def finish(tile, value):
        here = slice(tile * 128, (tile + 1) * 128)
        first = (-tile * 128) % (NB + 1)
        on_diagonal = jnp.logical_or(lane == first, lane == first + NB + 1)
        value = -0.5 * value - number * dens[:, here].astype(F32)
        out[:, here] = value + jnp.where(on_diagonal, half_number, 0.0)

    for quad in range(NB // 4):
        row_0 = matrix_row(4 * quad)
        row_1 = pltpu.roll(matrix_row(4 * quad + 1), 96, 1)
        row_2 = pltpu.roll(matrix_row(4 * quad + 2), 64, 1)
        row_3 = pltpu.roll(matrix_row(4 * quad + 3), 32, 1)
        finish(3 * quad, jnp.where(lane < 96, row_0, row_1))
        finish(3 * quad + 1, jnp.where(lane < 64, row_1, row_2))
        finish(3 * quad + 2, jnp.where(lane < 32, row_2, row_3))

    energy = jnp.zeros((1, 128), F32)
    for member in range(N_TEAM):
        start = member * 8 * PARTS + 16
        energy += arrived[start : start + 1, :]
    total[0] = jnp.sum(energy[:, SUM_LANE : SUM_LANE + 1])


def unpack_blocks(arrived, density, energies):
    return pl.pallas_call(
        unpack_kernel,
        out_shape=(
            jax.ShapeDtypeStruct((FRAG_DEV, FLAT), F32),
            jax.ShapeDtypeStruct((1,), F32),
            jax.ShapeDtypeStruct((DIM_DEV,), F32),
        ),
        in_specs=[pl.BlockSpec(memory_space=VMEM)] * 3,
        out_specs=(
            pl.BlockSpec(memory_space=VMEM),
            pl.BlockSpec(memory_space=SMEM),
            pl.BlockSpec(memory_space=SMEM),
        ),
        scratch_shapes=[VMEM((8 * NB, 128), F32)],
        compiler_params=pltpu.CompilerParams(vmem_limit_bytes=4 << 20),
        name="unpack_blocks",
    )(arrived.reshape(N_TEAM * 8 * PARTS, 128), density, energies)


def energy_moves():
    moves = []
    for group in range(N_GRP):
        for pair in range(N_PAIR):
            for core in range(2):
                source = group * N_FRAG + pair * 2 + core
                away = (pair + 2 * group + core) % N_PAIR
                moves.append((source, group * N_FRAG + away * 2 + core))
    return moves


def per_device(density, fock_blocks, coupling, dimer_pairs, atom_counts, nuclear_charge, coords):
    table, packed = atom_table(density, fock_blocks, nuclear_charge, atom_counts, coords)
    focks = [packed]
    for distance in range(1, REACH + 1):
        moves = [(index + distance, index) for index in range(N_FRAG - distance)]
        focks.append(lax.ppermute(packed, FRAG, moves))
    table = exchange(table, FRAG)
    fixed, starts = prepare_dimers(dimer_pairs, table, fock_blocks, coupling)
    sent, energies = solve_dimers(dimer_pairs, fixed, starts, focks)
    arrived = exchange(sent.reshape(N_TEAM, 8 * PARTS, 128), TEAM)
    own, next_1, next_2, energy = sort_blocks(arrived)
    from_1 = lax.ppermute(next_1, PAIR, [(index, index + 1) for index in range(N_PAIR - 1)])
    from_2 = lax.ppermute(next_2, PAIR, [(index, index + 2) for index in range(N_PAIR - 2)])
    energy = lax.ppermute(energy, GRP_FRAG, energy_moves())
    arrived = exchange(join_blocks(own, from_1, from_2, energy), TEAM)
    correction, total, energies = unpack_blocks(arrived, density, energies)
    return correction, energies, total.reshape(())


def solution(mesh):
    finer = Mesh(
        mesh.devices.reshape(2, 4, 2, 8, 2), ("grp_0", "grp_1", "frag_0", "frag_1", "frag_2")
    )
    return jax.shard_map(
        per_device,
        mesh=finer,
        in_specs=(
            P(FRAG, None),
            P(FRAG, None),
            P(GRP_FRAG, None),
            P(GRP_FRAG, None),
            P(FRAG),
            P(FRAG),
            P(None, FRAG),
        ),
        out_specs=(P(FRAG, None), P(GRP_FRAG), P()),
        check_vma=False,
    )
```
